32 devices in a mesh: ctx: 8 (over z, x), exp: 4 (over y, core).
Axes of the slice: x: 2, y: 2, z: 4, core: 2. Of those that a mesh axis runs over, the one named last changes fastest.
Arguments:
- queries: bfloat16 [1024, 4096], P('ctx', 'exp'), may hold values from -5 to 5
- keys: bfloat16 [1024, 1024], P('ctx', 'exp'), may hold values from -5 to 5
- values: bfloat16 [1024, 1024], P('ctx', 'exp'), may hold values from -6 to 6
- resid_in: bfloat16 [1024, 4096], P(('ctx', 'exp')), may hold values from -6 to 6
- span_order: int32 [16], replicated, may hold values from 0 to 15, each once
- out_weight: bfloat16 [4096, 4096], P('exp'), may hold values from -0.09375 to 0.09375
- norm_gain: float32 [4096], replicated, may hold values from 0.25 to 1.75
- router: float32 [4096, 4], replicated, may hold values from -0.09375 to 0.09375
- expert_ids: int32 [1024, 2], P(('ctx', 'exp')), may hold values from 0 to 3, all different within a row; in each aligned block of 32 rows (0 to 31, 32 to 63, ...) at most 16 rows name the same one
- w_gate: bfloat16 [4, 4096, 14336], P('exp', None, 'ctx'), may hold values from -0.09375 to 0.09375
- w_up: bfloat16 [4, 4096, 14336], P('exp', None, 'ctx'), may hold values from -0.09375 to 0.09375
- w_down: bfloat16 [4, 14336, 4096], P('exp', 'ctx'), may hold values from -0.046875 to 0.046875
Outputs:
- mixed: bfloat16 [1024, 4096], P(('ctx', 'exp'))
The draws below stay inside these ranges and needn't reach their ends.
Inputs may be any that keep to these rules, and one draw needn't show every extreme that they name: `expert_ids`: A token's 2 ids differ. In every aligned block of 32 tokens, each of the 4 experts is named by exactly 16 tokens. `span_order`: each span number appears once.
All inputs are finite; a program needn't handle non-finite values.
Results may differ from the reference program's by a relative error of at most 0.012.
Values may be sent and summed in bfloat16 or wider, within the bound.
A program may use at most 128 MiB of HBM per device.

```python
import math
import jax
import jax.numpy as jnp
import numpy as np
from jax import lax

D = 4096
QUERY_HEADS = 32
KEY_VALUE_HEADS = 8
HEAD_SIZE = 128
FF = 14336
TOP = 2
SPAN = 64
EXPERTS = 4
SEQUENCE_TOKENS = 1024
SPANS = 16
SUB = 32
SLOT = 16
N_CTX = 8


def base_domain(key, salt, columns):
    return jnp.clip(jax.random.normal(jax.random.fold_in(key, salt), (SEQUENCE_TOKENS, columns), jnp.float32), -5.0, 5.0)


def with_labels(key, field):
    return field


def draw_queries(key, part):
    return with_labels(key, base_domain(key, 11, QUERY_HEADS * HEAD_SIZE)).astype(jnp.bfloat16)


def draw_keys(key, part):
    return with_labels(key, base_domain(key, 23, KEY_VALUE_HEADS * HEAD_SIZE)).astype(jnp.bfloat16)


def steps_of(stream_key, extent, cuts, low, largest):
    def one(axis_at, parts):
        steps = jax.random.uniform(jax.random.fold_in(jax.random.fold_in(stream_key, 6), axis_at), (parts,), jnp.float32, low / len(cuts), largest / len(cuts))
        return jnp.repeat(jnp.exp(steps), extent[axis_at] // parts).reshape((-1,) + (1,) * (len(extent) - axis_at - 1))

    factor_of = one(*cuts[0])
    for cut in cuts[1:]:
        factor_of = factor_of * one(*cut)
    return factor_of


def assign_block(own_key, own, number, rows, number_of, top, limit, slope):
    ranking = jax.random.permutation(own_key, number_of)
    heavy_load, common = load_shares(number_of, rows * top, limit, slope, True), load_shares(number_of, rows * top, limit, slope, False)
    places = jnp.arange(number_of)

    def named(tallies, turn):
        used = int((tallies > 0).sum())
        fixed = max(1, used // 4)
        shifted = fixed + (places - fixed + turn * (used - fixed)) % max(1, number_of - fixed)
        return jnp.zeros((number_of,), jnp.int32).at[ranking[jnp.where(places < fixed, places, shifted)]].set(jnp.asarray(tallies, jnp.int32))

    tallies = jnp.where(number % 4 == 0, named(heavy_load, number // 4), named(common, number - number // 4 - 1))
    mixed = jax.random.permutation(jax.random.fold_in(own, 3), number_of)
    giver, sink = mixed[0:number_of // 2 * 2:2], mixed[1:number_of // 2 * 2:2]
    room = jnp.minimum(tallies[giver] - 1, limit - tallies[sink]) // 2
    room = jnp.where((giver == ranking[0]) | (sink == ranking[0]) | (tallies[sink] == 0), 0, jnp.maximum(room, 0))
    shifted = jax.random.randint(jax.random.fold_in(own, 4), (number_of // 2,), 0, 1 << 20) % (room + 1)
    tallies = tallies.at[giver].add(-shifted).at[sink].add(shifted)
    items = jnp.searchsorted(jnp.cumsum(tallies), jnp.arange(rows * top), side="right").astype(jnp.int32)
    listing = items.reshape(top, rows).T
    listing = listing[jax.random.permutation(jax.random.fold_in(own, 1), rows)]
    turn = jax.random.randint(jax.random.fold_in(own, 2), (rows, 1), 0, top)
    return jnp.take_along_axis(listing, (jnp.arange(top)[None, :] + turn) % top, axis=1)


def load_shares(number_of, total, reach, slope, full):
    loads = [(1 << 20) // math.isqrt(rank ** slope) + 1 for rank in range(1, number_of + 1)]
    largest = reach if full else min(reach, max(-(-total // number_of), total * loads[0] // sum(loads)))
    least = 1 if total - largest >= number_of - 1 else 0
    counts, rest = [largest] + [least] * (number_of - 1), total - largest - least * (number_of - 1)
    while rest > 0:
        movable = [i for i in range(1, number_of) if counts[i] < largest] or [i for i in range(1, number_of) if counts[i] < reach]
        whole, left = sum([loads[i] for i in movable]), rest
        for i in movable:
            more = min(reach - counts[i], max(1, left * loads[i] // whole), rest)
            counts[i] = counts[i] + more
            rest = rest - more
    return np.array(counts)


def normal_values(rng, dims, deviation, most, cuts=(), kind=jnp.bfloat16):
    level = steps_of(rng, dims, cuts, -0.22, 0.18) if cuts else 1.0
    entries = jax.random.normal(rng, dims, jnp.float32) * deviation * level
    return jnp.minimum(jnp.maximum(entries, -most), most).astype(kind)


def setup_inputs(seed: int = 0) -> dict:
    arg_keys = jax.random.split(jax.random.key(seed), 13)
    queries = draw_queries(jax.random.fold_in(arg_keys[12], 71), 0)
    keys = draw_keys(jax.random.fold_in(arg_keys[12], 71), 0)
    values = normal_values(arg_keys[2], (SEQUENCE_TOKENS, KEY_VALUE_HEADS * HEAD_SIZE), 1.0, 6.0, ((0, 8), (1, 4)))
    resid_in = normal_values(arg_keys[3], (SEQUENCE_TOKENS, D), 1.0, 6.0, ((0, 32),))
    span_order = jax.random.permutation(arg_keys[4], SPANS).astype(jnp.int32)
    out_weight = normal_values(arg_keys[5], (QUERY_HEADS * HEAD_SIZE, D), (QUERY_HEADS * HEAD_SIZE) ** -0.5, 0.09375, ((0, 4),))
    norm_gain = jnp.clip(1.0 + 0.15 * jax.random.normal(arg_keys[6], (D,), jnp.float32), 0.25, 1.75)
    router = normal_values(arg_keys[7], (D, EXPERTS), D ** -0.5, 0.09375, (), jnp.float32)
    expert_ids_keys = jax.random.split(jax.random.fold_in(arg_keys[8], 1), SEQUENCE_TOKENS // SUB)
    expert_ids_turns = jax.random.permutation(jax.random.fold_in(arg_keys[8], 3), SEQUENCE_TOKENS // SUB)
    expert_ids = jax.vmap(lambda own, number: assign_block(jax.random.fold_in(arg_keys[8], 2), own, number, SUB, EXPERTS, TOP, SLOT, 0))(expert_ids_keys, expert_ids_turns).reshape((SEQUENCE_TOKENS, TOP))
    w_gate = normal_values(arg_keys[9], (EXPERTS, D, FF), D ** -0.5, 0.09375, ((0, 4), (2, 8)))
    w_up = normal_values(arg_keys[10], (EXPERTS, D, FF), D ** -0.5, 0.09375, ((0, 4), (2, 8)))
    w_down = normal_values(arg_keys[11], (EXPERTS, FF, D), FF ** -0.5, 0.046875, ((0, 4), (1, 8)))
    return {"queries": queries, "keys": keys, "values": values, "resid_in": resid_in, "span_order": span_order, "out_weight": out_weight, "norm_gain": norm_gain, "router": router, "expert_ids": expert_ids, "w_gate": w_gate, "w_up": w_up, "w_down": w_down}


def expert_rows(inputs, gate_mat, up_mat, down_mat):
    shard_width = FF // N_CTX

    def add_shard(summed, shard_no):
        offset = (shard_no * shard_width).astype(jnp.int32)
        gate_part = jnp.dot(inputs, lax.dynamic_slice_in_dim(gate_mat, offset, shard_width, 1), preferred_element_type=jnp.float32)
        up_part = jnp.dot(inputs, lax.dynamic_slice_in_dim(up_mat, offset, shard_width, 1), preferred_element_type=jnp.float32)
        hidden = (jax.nn.silu(gate_part) * up_part).astype(jnp.bfloat16)
        partial_out = jnp.dot(hidden, lax.dynamic_slice_in_dim(down_mat, offset, shard_width, 0), preferred_element_type=jnp.float32)
        rounded = lax.optimization_barrier(partial_out.astype(jnp.bfloat16))
        return (summed + rounded.astype(jnp.float32), None)
    start_sum = jnp.zeros((inputs.shape[0], D), jnp.float32)
    summed, _ = lax.scan(add_shard, start_sum, jnp.arange(N_CTX, dtype=jnp.int32))
    return summed.astype(jnp.bfloat16)

def reference(queries, keys, values, resid_in, span_order, out_weight, norm_gain, router, expert_ids, w_gate, w_up, w_down):
    stored = jnp.arange(SEQUENCE_TOKENS, dtype=jnp.int32)
    position = span_order[stored // SPAN] * SPAN + stored % SPAN
    allowed = position[None, :] <= position[:, None]
    head_cluster = QUERY_HEADS // KEY_VALUE_HEADS
    query_head_rows = jnp.transpose(queries.astype(jnp.float32).reshape(SEQUENCE_TOKENS, KEY_VALUE_HEADS, head_cluster, HEAD_SIZE), (1, 2, 0, 3))
    key_head_rows = jnp.transpose(keys.astype(jnp.float32).reshape(SEQUENCE_TOKENS, KEY_VALUE_HEADS, HEAD_SIZE), (1, 0, 2))
    value_head_rows = jnp.transpose(values.astype(jnp.float32).reshape(SEQUENCE_TOKENS, KEY_VALUE_HEADS, HEAD_SIZE), (1, 0, 2))

    def one_head(operands):
        query_one, key_one, value_one = operands
        scores = jnp.einsum('gqd,kd->gqk', query_one, key_one) / math.sqrt(HEAD_SIZE)
        scores = jnp.where(allowed[None], scores, -1e+30)
        row_max = lax.optimization_barrier(jnp.max(scores, axis=-1, keepdims=True))
        weights = jnp.where(allowed[None], jnp.exp(scores - row_max), 0.0)
        denominator = lax.optimization_barrier(jnp.sum(weights, axis=-1))
        rounded = lax.optimization_barrier(weights.astype(jnp.bfloat16)).astype(jnp.float32)
        numerator = jnp.einsum('gqk,kd->gqd', rounded, value_one)
        return numerator / denominator[..., None]
    heads_out = lax.map(one_head, (query_head_rows, key_head_rows, value_head_rows))
    attended = jnp.transpose(heads_out, (2, 0, 1, 3)).reshape(SEQUENCE_TOKENS, QUERY_HEADS * HEAD_SIZE).astype(jnp.bfloat16)
    projected = jnp.dot(attended, out_weight, preferred_element_type=jnp.float32)
    stream = (resid_in.astype(jnp.float32) + projected).astype(jnp.bfloat16)
    stream_wide = stream.astype(jnp.float32)
    mean_square = lax.optimization_barrier(jnp.mean(stream_wide * stream_wide, axis=-1, keepdims=True))
    normed = (stream_wide * lax.rsqrt(mean_square + 1e-05) * norm_gain).astype(jnp.bfloat16)
    logits = jnp.dot(normed.astype(jnp.float32), router, precision=lax.Precision.HIGHEST)
    chosen = jnp.take_along_axis(logits, expert_ids, axis=1)
    mixing = jax.nn.softmax(chosen, axis=-1)
    expert_total = jnp.zeros((SEQUENCE_TOKENS, D), jnp.float32)
    row_count = SEQUENCE_TOKENS * TOP // EXPERTS
    for expert in range(EXPERTS):
        matches = expert_ids == expert
        routed = jnp.any(matches, axis=1)
        token_weight = lax.optimization_barrier(jnp.sum(jnp.where(matches, mixing, 0.0), axis=1))
        indices = jnp.nonzero(routed, size=row_count)[0].astype(jnp.int32)
        outputs = expert_rows(normed[indices], w_gate[expert], w_up[expert], w_down[expert])
        expert_total = expert_total.at[indices].add(token_weight[indices][:, None] * outputs.astype(jnp.float32))
    return (stream_wide + expert_total).astype(jnp.bfloat16)
```

```python
import functools
import math

import jax
import jax.numpy as jnp
from jax import lax
from jax.experimental import pallas as pl
from jax.experimental.pallas import tpu as pltpu
from jax.sharding import PartitionSpec as P

HEAD_SIZE = 128
SPAN = 64


def true_positions(row_ids, span_order):
    span_ids = jnp.arange(span_order.shape[0], dtype=jnp.int32)
    matches = (row_ids // SPAN)[:, None] == span_ids[None, :]
    return jnp.sum(jnp.where(matches, span_order[None, :], 0), axis=1) * SPAN + row_ids % SPAN


def on_device_xla(
    queries,
    keys,
    values,
    resid_in,
    span_order,
    out_weight,
    norm_gain,
    router,
    expert_ids,
    w_gate,
    w_up,
    w_down,
):
    tok_rows = queries.shape[0]
    kv_heads = keys.shape[1] // HEAD_SIZE
    head_cluster = queries.shape[1] // HEAD_SIZE // kv_heads
    ctx_index = lax.axis_index("ctx")
    query_pos = true_positions(
        ctx_index * tok_rows + jnp.arange(tok_rows, dtype=jnp.int32), span_order
    )
    shaped_queries = queries.reshape(tok_rows, kv_heads, head_cluster, HEAD_SIZE)
    score_scale = 1.0 / math.sqrt(HEAD_SIZE)
    pieces = (
        lax.all_gather(keys, "ctx", axis=0, tiled=True),
        lax.all_gather(values, "ctx", axis=0, tiled=True),
    )
    key_pos = true_positions(jnp.arange(pieces[0].shape[0], dtype=jnp.int32), span_order)
    running_max = jnp.full((kv_heads, head_cluster, tok_rows), -1e30, jnp.float32)
    key_block, value_block = pieces
    key_count = key_block.shape[0]
    key_head_rows = key_block.reshape(key_count, kv_heads, HEAD_SIZE)
    value_head_rows = value_block.reshape(key_count, kv_heads, HEAD_SIZE)
    scores = jnp.einsum(
        "qhgd,khd->hgqk", shaped_queries, key_head_rows, preferred_element_type=jnp.float32
    )
    allowed = key_pos[None, :] <= query_pos[:, None]
    scores = jnp.where(allowed[None, None], scores * score_scale, -1e30)
    new_max = jnp.maximum(running_max, jnp.max(scores, axis=-1))
    weights = jnp.where(allowed[None, None], jnp.exp(scores - new_max[..., None]), 0.0)
    running_sum = jnp.sum(weights, axis=-1)
    update = jnp.einsum(
        "hgqk,khd->qhgd",
        weights.astype(jnp.bfloat16),
        value_head_rows,
        preferred_element_type=jnp.float32,
    )
    weighted = update
    running_max, running_sum, weighted = (new_max, running_sum, weighted)
    attended = (
        (weighted / jnp.transpose(running_sum, (2, 0, 1))[..., None])
        .astype(jnp.bfloat16)
        .reshape(tok_rows, -1)
    )
    projected = jnp.dot(attended, out_weight, preferred_element_type=jnp.float32)
    own_sum = lax.psum_scatter(
        projected.astype(jnp.bfloat16), "exp", scatter_dimension=0, tiled=True
    ).astype(jnp.float32)
    stream = (resid_in.astype(jnp.float32) + own_sum).astype(jnp.bfloat16)
    stream_wide = stream.astype(jnp.float32)
    mean_square = jnp.mean(stream_wide * stream_wide, axis=-1, keepdims=True)
    normed = (stream_wide * lax.rsqrt(mean_square + 1e-05) * norm_gain).astype(jnp.bfloat16)
    model_dim = normed.shape[1]
    logits = jnp.dot(normed.astype(jnp.float32), router, precision=lax.Precision.HIGHEST)
    experts = router.shape[1]
    expert_axis = jnp.arange(experts, dtype=jnp.int32)
    picked = expert_ids[:, :, None] == expert_axis[None, None, :]
    chosen = jnp.sum(jnp.where(picked, logits[:, None, :], 0.0), axis=-1)
    mixing = jax.nn.softmax(chosen, axis=-1)
    token_weight = jnp.sum(jnp.where(picked, mixing[:, :, None], 0.0), axis=1)
    routed = jnp.any(picked, axis=1)
    rank_of = jnp.cumsum(routed.astype(jnp.int32), axis=0) - 1
    slot_count = resid_in.shape[0] * expert_ids.shape[1] // experts
    slot_axis = jnp.arange(slot_count, dtype=jnp.int32)
    placing = jnp.logical_and(
        routed.T[:, None, :], rank_of.T[:, None, :] == slot_axis[None, :, None]
    )
    outgoing = jnp.einsum(
        "est,td->esd", placing.astype(jnp.bfloat16), normed, preferred_element_type=jnp.float32
    ).astype(jnp.bfloat16)
    arrived = lax.all_to_all(outgoing, "exp", split_axis=0, concat_axis=0, tiled=True)
    rows_in = lax.all_gather(arrived.reshape(-1, model_dim), "ctx", axis=0, tiled=True)
    gate_part = jnp.dot(rows_in, w_gate[0], preferred_element_type=jnp.float32)
    up_part = jnp.dot(rows_in, w_up[0], preferred_element_type=jnp.float32)
    hidden = (jax.nn.silu(gate_part) * up_part).astype(jnp.bfloat16)
    partials = jnp.dot(hidden, w_down[0], preferred_element_type=jnp.float32)
    own_rows = lax.psum_scatter(
        partials.astype(jnp.bfloat16), "ctx", scatter_dimension=0, tiled=True
    )
    results = own_rows.reshape(experts, slot_count, model_dim)
    returned = lax.all_to_all(results, "exp", split_axis=0, concat_axis=0, tiled=True)
    coefficient = placing.astype(jnp.float32) * token_weight.T[:, None, :]
    combined = jnp.einsum("est,esd->td", coefficient, returned.astype(jnp.float32))
    return (stream_wide + combined).astype(jnp.bfloat16)


VMEM_BYTES = 60 * 2**20
LOAD_ROWS = 512
MESH = pl.DeviceIdType.MESH


def place_of():
    ctx, exp = lax.axis_index("ctx"), lax.axis_index("exp")
    return ctx // 2, ctx % 2, exp // 2, exp % 2


def at(z, x, y, c):
    return (z * 2 + x, y * 2 + c)


def level_at(z, turn, levels):
    upper = z // (levels // 2)
    sign = 1 - 2 * upper
    inner = z * (1 - upper) + (levels - 1 - z) * upper
    beyond = jnp.minimum(jnp.maximum(turn - 2 * inner, 0), 1)
    step = (turn + 1) // 2 * (1 if turn % 2 else -1)
    return z + sign * ((1 - beyond) * step + beyond * (turn - inner))


def greet(devices):
    barrier = pltpu.get_barrier_semaphore()
    for device in devices:
        pl.semaphore_signal(barrier, inc=1, device_id=device, device_id_type=MESH)
    pl.semaphore_wait(barrier, len(devices))


def start_send(src, dst, send_sem, recv_sem, device):
    copy = pltpu.make_async_remote_copy(
        src_ref=src,
        dst_ref=dst,
        send_sem=send_sem,
        recv_sem=recv_sem,
        device_id=device,
        device_id_type=MESH,
    )
    copy.start()
    return copy


def gather_keys_kernel(levels, k_ref, v_ref, ko_ref, vo_ref, zs, zr, xs, xr):
    z, x, y, c = place_of()
    greet([at((z + d) % levels, x, y, c) for d in range(1, levels)] + [at(z, 1 - x, y, c)])
    x_peer = at(z, 1 - x, y, c)
    mine = z * 2 + x
    z_copies, x_copies = [], []
    pairs = ((k_ref, ko_ref), (v_ref, vo_ref))
    for d in range(1, levels):
        for i, (own, out) in enumerate(pairs):
            z_copies.append(
                start_send(own, out.at[mine], zs.at[i, d], zr.at[i, d], at((z + d) % levels, x, y, c))
            )
    for i, (own, out) in enumerate(pairs):
        x_copies.append(start_send(own, out.at[mine], xs.at[i, 0], xr.at[i, 0], x_peer))
    for own, out in pairs:
        out[mine] = own[...]
    for d in range(1, levels):
        block = (z + levels - d) % levels * 2 + x
        for i, (own, out) in enumerate(pairs):
            z_copies[(d - 1) * 2 + i].wait_recv()
            x_copies.append(
                start_send(out.at[block], out.at[block], xs.at[i, d], xr.at[i, d], x_peer)
            )
    for copy in x_copies:
        copy.wait_recv()
    for copy in z_copies + x_copies:
        copy.wait_send()


def gather_keys(keys, values, levels):
    shape = jax.ShapeDtypeStruct((levels * 2,) + keys.shape, keys.dtype)
    vmem = pl.BlockSpec(memory_space=pltpu.VMEM)
    sems = pltpu.SemaphoreType.DMA((2, levels))
    return pl.pallas_call(
        functools.partial(gather_keys_kernel, levels),
        out_shape=(shape, shape),
        in_specs=[vmem] * 2,
        out_specs=(vmem, vmem),
        scratch_shapes=[sems] * 4,
        compiler_params=pltpu.CompilerParams(collective_id=0, has_side_effects=True),
    )(keys, values)


def stream_kernel(
    levels, sub, model, half, experts, slots, tile, proj_ref, resid_ref, gain_ref, router_ref,
    ids_ref, gate_ref, up_ref, stream_ref, hidden_ref, placing_ref, weight_ref,
    out_ref, gate_w, up_w, rows_ref,
    kept, from_core, from_y, ss, rs, zs, zr, xs, xr, ys, yr, ds, dr, es, er, cs, cr, gs, us,
):
    loads = []
    for part in range(model // LOAD_ROWS):
        rows = slice(part * LOAD_ROWS, (part + 1) * LOAD_ROWS)
        loads.append(pltpu.make_async_copy(gate_ref.at[0, rows], gate_w.at[rows], gs.at[part]))
        loads.append(pltpu.make_async_copy(up_ref.at[0, rows], up_w.at[rows], us.at[part]))
    for load in loads:
        load.start()
    z, x, y, c = place_of()
    x_peer, y_peer, c_peer = at(z, 1 - x, y, c), at(z, x, 1 - y, c), at(z, x, y, 1 - c)
    z_peers = [at((z + d) % levels, x, y, c) for d in range(1, levels)]
    greet(z_peers + [x_peer, y_peer, c_peer])

    order = (1 - y, y)
    first = [
        start_send(proj_ref.at[row, 1 - c], from_core.at[i], ss.at[i], rs.at[i], c_peer)
        for i, row in enumerate(order)
    ]
    first[0].wait_recv()
    kept[0] = (
        proj_ref[1 - y, c].astype(jnp.float32) + from_core[0].astype(jnp.float32)
    ).astype(jnp.bfloat16)
    second = start_send(kept.at[0], from_y, ss.at[2], rs.at[2], y_peer)
    first[1].wait_recv()
    total = proj_ref[y, c].astype(jnp.float32) + from_core[1].astype(jnp.float32)
    total = total + resid_ref[...].astype(jnp.float32)
    second.wait_recv()
    stream = (total + from_y[...].astype(jnp.float32)).astype(jnp.bfloat16)
    stream_ref[...] = stream
    wide = stream.astype(jnp.float32)
    mean_square = jnp.mean(wide * wide, axis=-1, keepdims=True)
    normed = (wide * lax.rsqrt(mean_square + 1e-05) * gain_ref[...]).astype(jnp.bfloat16)

    normed_wide = normed.astype(jnp.float32)
    logits = [
        jnp.sum(normed_wide * router_ref[e : e + 1, :], axis=-1, keepdims=True)
        for e in range(experts)
    ]
    ids = ids_ref[...]
    id0, id1 = ids[:, 0:1], ids[:, 1:2]
    zero = jnp.zeros_like(logits[0])
    pick0, pick1 = zero, zero
    for e in range(experts):
        pick0 = pick0 + jnp.where(id0 == e, logits[e], 0.0)
        pick1 = pick1 + jnp.where(id1 == e, logits[e], 0.0)
    top = jnp.maximum(pick0, pick1)
    exp0, exp1 = jnp.exp(pick0 - top), jnp.exp(pick1 - top)
    gate0, gate1 = exp0 / (exp0 + exp1), exp1 / (exp0 + exp1)
    lane = lax.broadcasted_iota(jnp.int32, (sub, 128), 1)
    expert = lane % experts
    routed = jnp.logical_or(expert == id0, expert == id1)
    weight = jnp.where(expert == id0, gate0, 0.0) + jnp.where(expert == id1, gate1, 0.0)
    high = weight.astype(jnp.bfloat16).astype(jnp.float32)
    group = lane // experts
    tail = jnp.where(
        group == 0,
        jnp.where(routed, 1.0, 0.0),
        jnp.where(group == 1, high, jnp.where(group == 2, weight - high, 0.0)),
    )

    def block(k, bx, by):
        return ((k * 2 + bx) * 2 + by) * 2 + c

    mine = block(z, x, y)
    out_ref[mine, :, 0:model] = normed
    out_ref[mine, :, model : model + 128] = tail.astype(jnp.bfloat16)

    left, right = slice(0, half), slice(half, model + 128)
    copies = [second] + first
    z_sides = ((1, z < levels - 1), (-1, z > 0))

    def z_copy(side, k):
        ref = out_ref.at[block(k, x, y)]
        return pltpu.make_async_remote_copy(
            src_ref=ref,
            dst_ref=ref,
            send_sem=zs.at[side, k],
            recv_sem=zr.at[k],
            device_id=at(z + z_sides[side][0], x, y, c),
            device_id_type=MESH,
        )

    def z_pass(k, whole):
        for side, (step, there) in enumerate(z_sides):
            behind = (z - k) * step

            @pl.when(jnp.logical_and(there, behind >= 0 if whole else behind > 0))
            def _():
                z_copy(side, k).start()

    z_pass(z, True)
    at_end = z % (levels - 1) == 0
    x_copies, y_copies, d_copies, e_copies, c_copies = [], [], [], [], []

    def to_core(index):
        n = len(c_copies)
        ref = out_ref.at[index]
        c_copies.append(start_send(ref, ref, cs.at[n], cr.at[n], c_peer))
        return n

    sent = {d: [] for d in range(levels)}

    def finish(d):
        k = level_at(z, d, levels)
        d_copies[d].wait_recv()
        e_copies[d].wait_recv()
        sent[d].append(to_core(block(k, 1 - x, 1 - y)))

    mine_expert = lax.axis_index("exp")
    count = 8 * sub

    def experts_of(d):
        k = level_at(z, d, levels)
        for n in sent[d]:
            c_copies[n].wait_recv()
        info = out_ref[pl.ds(k * 8, 8), :, model : model + 128].reshape(count, 128)
        above = lax.broadcasted_iota(jnp.int32, (count, count), 0)
        below = lax.broadcasted_iota(jnp.int32, (count, count), 1)
        within = jnp.logical_and(above // sub == below // sub, below <= above)
        seen = jnp.dot(
            jnp.where(within, 1.0, 0.0).astype(jnp.bfloat16),
            info,
            preferred_element_type=jnp.float32,
        )
        wide_info = info.astype(jnp.float32)
        at_lane = lax.broadcasted_iota(jnp.int32, (count, 128), 1)

        def lane_sum(value, keep):
            return jnp.sum(jnp.where(keep, value, 0.0), axis=1, keepdims=True)

        is_mine = at_lane == mine_expert
        here = lane_sum(wide_info, is_mine)
        rank = lane_sum(seen, is_mine).astype(jnp.int32) - 1
        token_weight = lane_sum(
            wide_info,
            jnp.logical_or(at_lane == experts + mine_expert, at_lane == 2 * experts + mine_expert),
        )
        token = lax.broadcasted_iota(jnp.int32, (count, 1), 0)
        slot = jnp.where(here > 0.5, token // sub * slots + rank, -1)
        at_slot = lax.broadcasted_iota(jnp.int32, (count, 8 * slots), 1)
        placing = jnp.where(at_slot == slot, 1.0, 0.0).astype(jnp.bfloat16)
        placing_ref[k] = placing
        weight_ref[k] = jnp.broadcast_to(token_weight, (count, 128))
        picked_rows = jnp.where(at_slot == slot, 1.0, 0.0).T.astype(jnp.bfloat16)

        def pick(j, carry):
            columns = pl.ds(pl.multiple_of(j * 1024, 1024), 1024)
            block_in = out_ref[pl.ds(k * 8, 8), :, columns].reshape(count, 1024)
            rows_ref[:, columns] = jnp.dot(
                picked_rows, block_in, preferred_element_type=jnp.float32
            ).astype(jnp.bfloat16)
            return carry

        lax.fori_loop(0, model // 1024, pick, 0)
        if d == 0:
            for load in loads:
                load.wait()

        def unit(j, carry):
            columns = pl.ds(pl.multiple_of(j * tile, tile), tile)
            rows = rows_ref[...]
            gate = jnp.dot(rows, gate_w[:, columns], preferred_element_type=jnp.float32)
            up = jnp.dot(rows, up_w[:, columns], preferred_element_type=jnp.float32)
            hidden_ref[k, :, columns] = (gate * jax.nn.sigmoid(gate) * up).astype(jnp.bfloat16)
            return carry

        lax.fori_loop(0, hidden_ref.shape[2] // tile, unit, 0)

    for turn in range(levels + 1):
        if turn < levels:
            k = level_at(z, turn, levels)
            if 0 < turn < levels - 1:
                z_copy(0, k).wait_recv()
                z_pass(k, False)
            elif turn:

                @pl.when(at_end)
                def _():
                    z_copy(0, k).wait_recv()

            ref = out_ref.at[block(k, x, y)]
            x_copies.append(start_send(ref, ref, xs.at[turn], xr.at[turn], x_peer))
            y_copies.append(start_send(ref, ref, ys.at[turn], yr.at[turn], y_peer))
            sent[turn].append(to_core(block(k, x, y)))
        if turn:
            d = turn - 1
            k = level_at(z, d, levels)
            x_copies[d].wait_recv()
            ref = out_ref.at[block(k, 1 - x, y), :, left]
            d_copies.append(start_send(ref, ref, ds.at[d], dr.at[d], y_peer))
            sent[d].append(to_core(block(k, 1 - x, y)))
            y_copies[d].wait_recv()
            ref = out_ref.at[block(k, x, 1 - y), :, right]
            e_copies.append(start_send(ref, ref, es.at[d], er.at[d], x_peer))
            sent[d].append(to_core(block(k, x, 1 - y)))
        if turn >= 2:
            finish(turn - 2)
            if turn == levels - 2:
                k = level_at(z, levels - 1, levels)

                @pl.when(jnp.logical_not(at_end))
                def _():
                    z_copy(0, k).wait_recv()
                    z_pass(k, False)

            experts_of(turn - 2)
    finish(levels - 1)
    experts_of(levels - 1)
    for copy in copies + x_copies + y_copies + d_copies + e_copies + c_copies:
        copy.wait_send()
    for k in range(levels):
        for side, (step, there) in enumerate(z_sides):

            @pl.when(jnp.logical_and(there, (z - k) * step >= 0))
            def _():
                z_copy(side, k).wait_send()


def stream_and_hidden(projected, resid_in, norm_gain, router, expert_ids, gate, up, levels):
    sub, model = resid_in.shape
    experts = router.shape[1]
    width = gate.shape[2]
    slots = sub * expert_ids.shape[1] // experts
    vmem = pl.BlockSpec(memory_space=pltpu.VMEM)
    hbm = pl.BlockSpec(memory_space=pl.ANY)
    dma = pltpu.SemaphoreType.DMA
    bf16 = jnp.bfloat16
    return pl.pallas_call(
        functools.partial(
            stream_kernel, levels, sub, model, model // 2, experts, slots, width // 2
        ),
        out_shape=(
            jax.ShapeDtypeStruct((sub, model), bf16),
            jax.ShapeDtypeStruct((levels, 8 * slots, width), bf16),
            jax.ShapeDtypeStruct((levels, 8 * sub, 8 * slots), bf16),
            jax.ShapeDtypeStruct((levels, 8 * sub, 128), jnp.float32),
        ),
        in_specs=[vmem] * 5 + [hbm] * 2,
        out_specs=(vmem,) * 4,
        scratch_shapes=[
            pltpu.VMEM((levels * 8, sub, model + 128), bf16),
            pltpu.VMEM((model, width), bf16),
            pltpu.VMEM((model, width), bf16),
            pltpu.VMEM((8 * slots, model), bf16),
            pltpu.VMEM((1, sub, model), bf16),
            pltpu.VMEM((2, sub, model), bf16),
            pltpu.VMEM((sub, model), bf16),
            dma((3,)),
            dma((3,)),
        ]
        + [dma((2, levels))]
        + [dma((levels,))] * 9
        + [dma((levels * 4,))] * 2
        + [dma((model // LOAD_ROWS,))] * 2,
        compiler_params=pltpu.CompilerParams(
            collective_id=1, has_side_effects=True, vmem_limit_bytes=VMEM_BYTES
        ),
    )(
        projected.reshape(2, 2, sub, model),
        resid_in,
        norm_gain.reshape(1, model),
        router.T,
        expert_ids,
        gate,
        up,
    )


def sum_kernel(
    levels, sub, model, half, tile, hidden_ref, placing_ref, weight_ref, down_ref, stream_ref,
    out_ref, part_ref, down_w, core_in, held, a_in, b_in, a2_in, b2_in, ready, z_in, total,
    cs, cr, sa, ra, sb, rb, sa2, ra2, sb2, rb2, zs, zr, ls,
):
    loads = []
    for j in range(model // tile):
        columns = slice(j * tile, (j + 1) * tile)
        loads.append(
            pltpu.make_async_copy(down_ref.at[0, :, columns], down_w.at[:, columns], ls.at[j])
        )
        loads[j].start()
    z, x, y, c = place_of()
    x_peer, y_peer, c_peer = at(z, 1 - x, y, c), at(z, x, 1 - y, c), at(z, x, y, 1 - c)
    z_peers = [at((z + d) % levels, x, y, c) for d in range(1, levels)]
    greet(z_peers + [x_peer, y_peer, c_peer])
    turns = list(range(levels))
    left, right = slice(0, half), slice(half, model)
    f32, bf16 = jnp.float32, jnp.bfloat16
    c_copies = [None] * levels

    def target(d):
        return level_at(z, levels - 1 - d, levels)

    def terms_of(d):
        k = target(d)
        lanes = weight_ref[k]
        weight = jnp.concatenate([lanes] * (tile // 128), axis=1)
        hidden = hidden_ref[k]
        placing = placing_ref[k]

        def one(columns):
            rows = jnp.dot(hidden, down_w[:, columns], preferred_element_type=f32).astype(bf16)
            spread = jnp.dot(placing, rows, preferred_element_type=f32)
            part_ref[k, :, :, :, :, columns] = (
                (spread * weight).astype(bf16).reshape(2, 2, 2, sub, tile)
            )

        if d == turns[0]:
            for j in range(model // tile):
                loads[j].wait()
                one(slice(j * tile, (j + 1) * tile))
        else:

            def looped(j, carry):
                one(pl.ds(pl.multiple_of(j * tile, tile), tile))
                return carry

            lax.fori_loop(0, model // tile, looped, 0)
        c_copies[d] = start_send(
            part_ref.at[k, :, :, 1 - c], core_in.at[d], cs.at[d], cr.at[d], c_peer
        )
    terms_of(turns[0])
    stage2, stage3 = {}, {}
    z_sides = ((1, z > 0), (-1, z < levels - 1))

    def z_copy(d, side):
        k = target(d)
        return pltpu.make_async_remote_copy(
            src_ref=ready.at[d],
            dst_ref=z_in.at[side, k],
            send_sem=zs.at[d],
            recv_sem=zr.at[side, k],
            device_id=at(z + z_sides[side][0], x, y, c),
            device_id_type=MESH,
        )

    def z_send(d, with_outer):
        ahead = target(d) - z
        for side, (step, outer) in enumerate(z_sides):
            right_way = ahead * step > 0

            @pl.when(jnp.logical_and(right_way, outer if with_outer else jnp.logical_not(outer)))
            def _():
                if with_outer:
                    z_copy(d, side).wait_recv()
                    ready[d] = (
                        ready[d].astype(f32) + z_in[side, target(d)].astype(f32)
                    ).astype(bf16)
                z_copy(d, side).start()

    for step in range(levels + 2):
        if step < levels:
            d = turns[step]
            k = target(d)
            c_copies[d].wait_recv()
            for bx in range(2):
                for by in range(2):
                    held[d, bx, by] = (
                        part_ref[k, bx, by, c].astype(f32) + core_in[d, bx, by].astype(f32)
                    ).astype(bf16)
            stage2[d] = (
                start_send(
                    held.at[d, :, 1 - y, :, left], a_in.at[d], sa.at[d], ra.at[d], y_peer
                ),
                start_send(
                    held.at[d, 1 - x, :, :, right], b_in.at[d], sb.at[d], rb.at[d], x_peer
                ),
            )
        if step + 1 < levels:
            terms_of(turns[step + 1])
        if 1 <= step <= levels:
            d = turns[step - 1]
            stage2[d][0].wait_recv()
            ready[d, :, left] = (
                held[d, 1 - x, y, :, left].astype(f32) + a_in[d, 1 - x].astype(f32)
            ).astype(bf16)
            stage2[d][1].wait_recv()
            ready[d, :, right] = (
                held[d, x, 1 - y, :, right].astype(f32) + b_in[d, 1 - y].astype(f32)
            ).astype(bf16)
            stage3[d] = (
                start_send(ready.at[d, :, left], a2_in.at[d], sa2.at[d], ra2.at[d], x_peer),
                start_send(ready.at[d, :, right], b2_in.at[d], sb2.at[d], rb2.at[d], y_peer),
            )
        if step >= 2:
            d = turns[step - 2]
            stage3[d][0].wait()
            stage3[d][1].wait()
            low = (
                held[d, x, y, :, left].astype(f32)
                + a_in[d, x].astype(f32)
                + a2_in[d].astype(f32)
            )
            high = (
                held[d, x, y, :, right].astype(f32)
                + b_in[d, y].astype(f32)
                + b2_in[d].astype(f32)
            )
            if d < levels - 1:
                ready[d, :, left] = low.astype(bf16)
                ready[d, :, right] = high.astype(bf16)
                z_send(d, False)
            else:
                total[:, left] = stream_ref[:, left].astype(f32) + low
                total[:, right] = stream_ref[:, right].astype(f32) + high
        for d in range(levels - 1):
            if step == (d + 3 if d < levels - 2 else d + 2):
                z_send(d, True)
    for side, (_, outer) in enumerate(z_sides):

        @pl.when(outer)
        def _():
            z_copy(levels - 1, side).wait_recv()
            total[...] += z_in[side, z].astype(f32)

    out_ref[...] = total[...].astype(bf16)
    for d in range(levels):
        c_copies[d].wait_send()
        for copy in stage2[d]:
            copy.wait_send()
        if d < levels - 1:
            z_copy(d, 0).wait_send()


def sum_terms(hidden, placing, weight, down, stream, levels):
    sub, model = stream.shape
    half = model // 2
    tile = 1024
    vmem = pl.BlockSpec(memory_space=pltpu.VMEM)
    dma = pltpu.SemaphoreType.DMA
    bf16 = jnp.bfloat16
    return pl.pallas_call(
        functools.partial(sum_kernel, levels, sub, model, half, tile),
        out_shape=jax.ShapeDtypeStruct((sub, model), bf16),
        in_specs=[vmem] * 3 + [pl.BlockSpec(memory_space=pl.ANY), vmem],
        out_specs=vmem,
        scratch_shapes=[
            pltpu.VMEM((levels, 2, 2, 2, sub, model), bf16),
            pltpu.VMEM(down.shape[1:], bf16),
            pltpu.VMEM((levels, 2, 2, sub, model), bf16),
            pltpu.VMEM((levels, 2, 2, sub, model), bf16),
            pltpu.VMEM((levels, 2, sub, half), bf16),
            pltpu.VMEM((levels, 2, sub, half), bf16),
            pltpu.VMEM((levels, sub, half), bf16),
            pltpu.VMEM((levels, sub, half), bf16),
            pltpu.VMEM((levels, sub, model), bf16),
            pltpu.VMEM((2, levels, sub, model), bf16),
            pltpu.VMEM((sub, model), jnp.float32),
        ]
        + [dma((levels,))] * 11
        + [dma((2, levels))]
        + [dma((model // tile,))],
        compiler_params=pltpu.CompilerParams(
            collective_id=2, has_side_effects=True, vmem_limit_bytes=VMEM_BYTES
        ),
    )(hidden, placing, weight, down, stream)


def on_device(
    levels,
    queries,
    keys,
    values,
    resid_in,
    span_order,
    out_weight,
    norm_gain,
    router,
    expert_ids,
    w_gate,
    w_up,
    w_down,
):
    tok_rows = queries.shape[0]
    kv_heads = keys.shape[1] // HEAD_SIZE
    head_cluster = queries.shape[1] // HEAD_SIZE // kv_heads
    ctx_index = lax.axis_index("ctx")
    query_pos = true_positions(
        ctx_index * tok_rows + jnp.arange(tok_rows, dtype=jnp.int32), span_order
    )
    shaped_queries = queries.reshape(tok_rows, kv_heads, head_cluster, HEAD_SIZE)
    score_scale = 1.0 / math.sqrt(HEAD_SIZE)
    all_keys, all_values = gather_keys(keys, values, levels)
    key_count = levels * 2 * tok_rows
    key_pos = true_positions(jnp.arange(key_count, dtype=jnp.int32), span_order)
    key_head_rows = all_keys.reshape(key_count, kv_heads, HEAD_SIZE)
    value_head_rows = all_values.reshape(key_count, kv_heads, HEAD_SIZE)
    scores = jnp.einsum(
        "qhgd,khd->hgqk", shaped_queries, key_head_rows, preferred_element_type=jnp.float32
    )
    allowed = key_pos[None, :] <= query_pos[:, None]
    scores = jnp.where(allowed[None, None], scores * score_scale, -1e30)
    row_max = jnp.max(scores, axis=-1)
    weights = jnp.where(allowed[None, None], jnp.exp(scores - row_max[..., None]), 0.0)
    row_sum = jnp.sum(weights, axis=-1)
    weighted = jnp.einsum(
        "hgqk,khd->qhgd",
        weights.astype(jnp.bfloat16),
        value_head_rows,
        preferred_element_type=jnp.float32,
    )
    attended = (
        (weighted / jnp.transpose(row_sum, (2, 0, 1))[..., None])
        .astype(jnp.bfloat16)
        .reshape(tok_rows, -1)
    )
    projected = jnp.dot(attended, out_weight, preferred_element_type=jnp.float32).astype(
        jnp.bfloat16
    )
    stream, hidden, placing, weight = stream_and_hidden(
        projected, resid_in, norm_gain, router, expert_ids, w_gate, w_up, levels
    )
    return sum_terms(hidden, placing, weight, w_down, stream, levels)


def solution(mesh):
    placed = (
        P("ctx", "exp"),
        P("ctx", "exp"),
        P("ctx", "exp"),
        P(("ctx", "exp"), None),
        P(),
        P("exp", None),
        P(),
        P(),
        P(("ctx", "exp"), None),
        P("exp", None, "ctx"),
        P("exp", None, "ctx"),
        P("exp", "ctx", None),
    )
    levels = mesh.shape["ctx"] // 2

    def body(queries, keys, values, resid_in, *rest):
        blocks = resid_in.size * mesh.size * 2
        small = mesh.shape["exp"] == 4 and levels == 4 and blocks * 4 <= VMEM_BYTES
        local = functools.partial(on_device, levels) if small else on_device_xla
        return local(queries, keys, values, resid_in, *rest)

    return jax.shard_map(
        body, mesh=mesh, in_specs=placed, out_specs=P(("ctx", "exp"), None), check_vma=False
    )
```

```python
import functools
import math

import jax
import jax.numpy as jnp
from jax import lax
from jax.experimental import pallas as pl
from jax.experimental.pallas import tpu as pltpu
from jax.sharding import PartitionSpec as P

HEAD_SIZE = 128
SPAN = 64


def true_positions(row_ids, span_order):
    span_ids = jnp.arange(span_order.shape[0], dtype=jnp.int32)
    matches = (row_ids // SPAN)[:, None] == span_ids[None, :]
    return jnp.sum(jnp.where(matches, span_order[None, :], 0), axis=1) * SPAN + row_ids % SPAN


def on_device_xla(
    queries,
    keys,
    values,
    resid_in,
    span_order,
    out_weight,
    norm_gain,
    router,
    expert_ids,
    w_gate,
    w_up,
    w_down,
):
    tok_rows = queries.shape[0]
    kv_heads = keys.shape[1] // HEAD_SIZE
    head_cluster = queries.shape[1] // HEAD_SIZE // kv_heads
    ctx_index = lax.axis_index("ctx")
    query_pos = true_positions(
        ctx_index * tok_rows + jnp.arange(tok_rows, dtype=jnp.int32), span_order
    )
    shaped_queries = queries.reshape(tok_rows, kv_heads, head_cluster, HEAD_SIZE)
    score_scale = 1.0 / math.sqrt(HEAD_SIZE)
    pieces = (
        lax.all_gather(keys, "ctx", axis=0, tiled=True),
        lax.all_gather(values, "ctx", axis=0, tiled=True),
    )
    key_pos = true_positions(jnp.arange(pieces[0].shape[0], dtype=jnp.int32), span_order)
    running_max = jnp.full((kv_heads, head_cluster, tok_rows), -1e30, jnp.float32)
    key_block, value_block = pieces
    key_count = key_block.shape[0]
    key_head_rows = key_block.reshape(key_count, kv_heads, HEAD_SIZE)
    value_head_rows = value_block.reshape(key_count, kv_heads, HEAD_SIZE)
    scores = jnp.einsum(
        "qhgd,khd->hgqk", shaped_queries, key_head_rows, preferred_element_type=jnp.float32
    )
    allowed = key_pos[None, :] <= query_pos[:, None]
    scores = jnp.where(allowed[None, None], scores * score_scale, -1e30)
    new_max = jnp.maximum(running_max, jnp.max(scores, axis=-1))
    weights = jnp.where(allowed[None, None], jnp.exp(scores - new_max[..., None]), 0.0)
    running_sum = jnp.sum(weights, axis=-1)
    update = jnp.einsum(
        "hgqk,khd->qhgd",
        weights.astype(jnp.bfloat16),
        value_head_rows,
        preferred_element_type=jnp.float32,
    )
    weighted = update
    running_max, running_sum, weighted = (new_max, running_sum, weighted)
    attended = (
        (weighted / jnp.transpose(running_sum, (2, 0, 1))[..., None])
        .astype(jnp.bfloat16)
        .reshape(tok_rows, -1)
    )
    projected = jnp.dot(attended, out_weight, preferred_element_type=jnp.float32)
    own_sum = lax.psum_scatter(
        projected.astype(jnp.bfloat16), "exp", scatter_dimension=0, tiled=True
    ).astype(jnp.float32)
    stream = (resid_in.astype(jnp.float32) + own_sum).astype(jnp.bfloat16)
    stream_wide = stream.astype(jnp.float32)
    mean_square = jnp.mean(stream_wide * stream_wide, axis=-1, keepdims=True)
    normed = (stream_wide * lax.rsqrt(mean_square + 1e-05) * norm_gain).astype(jnp.bfloat16)
    model_dim = normed.shape[1]
    logits = jnp.dot(normed.astype(jnp.float32), router, precision=lax.Precision.HIGHEST)
    experts = router.shape[1]
    expert_axis = jnp.arange(experts, dtype=jnp.int32)
    picked = expert_ids[:, :, None] == expert_axis[None, None, :]
    chosen = jnp.sum(jnp.where(picked, logits[:, None, :], 0.0), axis=-1)
    mixing = jax.nn.softmax(chosen, axis=-1)
    token_weight = jnp.sum(jnp.where(picked, mixing[:, :, None], 0.0), axis=1)
    routed = jnp.any(picked, axis=1)
    rank_of = jnp.cumsum(routed.astype(jnp.int32), axis=0) - 1
    slot_count = resid_in.shape[0] * expert_ids.shape[1] // experts
    slot_axis = jnp.arange(slot_count, dtype=jnp.int32)
    placing = jnp.logical_and(
        routed.T[:, None, :], rank_of.T[:, None, :] == slot_axis[None, :, None]
    )
    outgoing = jnp.einsum(
        "est,td->esd", placing.astype(jnp.bfloat16), normed, preferred_element_type=jnp.float32
    ).astype(jnp.bfloat16)
    arrived = lax.all_to_all(outgoing, "exp", split_axis=0, concat_axis=0, tiled=True)
    rows_in = lax.all_gather(arrived.reshape(-1, model_dim), "ctx", axis=0, tiled=True)
    gate_part = jnp.dot(rows_in, w_gate[0], preferred_element_type=jnp.float32)
    up_part = jnp.dot(rows_in, w_up[0], preferred_element_type=jnp.float32)
    hidden = (jax.nn.silu(gate_part) * up_part).astype(jnp.bfloat16)
    partials = jnp.dot(hidden, w_down[0], preferred_element_type=jnp.float32)
    own_rows = lax.psum_scatter(
        partials.astype(jnp.bfloat16), "ctx", scatter_dimension=0, tiled=True
    )
    results = own_rows.reshape(experts, slot_count, model_dim)
    returned = lax.all_to_all(results, "exp", split_axis=0, concat_axis=0, tiled=True)
    coefficient = placing.astype(jnp.float32) * token_weight.T[:, None, :]
    combined = jnp.einsum("est,esd->td", coefficient, returned.astype(jnp.float32))
    return (stream_wide + combined).astype(jnp.bfloat16)


VMEM_BYTES = 60 * 2**20
LOAD_ROWS = 512
MESH = pl.DeviceIdType.MESH


def place_of():
    ctx, exp = lax.axis_index("ctx"), lax.axis_index("exp")
    return ctx // 2, ctx % 2, exp // 2, exp % 2


def at(z, x, y, c):
    return (z * 2 + x, y * 2 + c)


def level_at(z, turn, levels):
    upper = z // (levels // 2)
    sign = 1 - 2 * upper
    inner = z * (1 - upper) + (levels - 1 - z) * upper
    beyond = jnp.minimum(jnp.maximum(turn - 2 * inner, 0), 1)
    step = (turn + 1) // 2 * (1 if turn % 2 else -1)
    return z + sign * ((1 - beyond) * step + beyond * (turn - inner))


def neighbours(z, x, y, c, levels):
    return (
        (at(z, 1 - x, y, c), None),
        (at(z, x, 1 - y, c), None),
        (at(z, x, y, 1 - c), None),
        (at(z - 1, x, y, c), z > 0),
        (at(z + 1, x, y, c), z < levels - 1),
    )


def announce(z, x, y, c, levels):
    barrier = pltpu.get_barrier_semaphore()
    for device, there in neighbours(z, x, y, c, levels):

        def signal():
            pl.semaphore_signal(barrier, inc=1, device_id=device, device_id_type=MESH)

        if there is None:
            signal()
        else:
            pl.when(there)(signal)


def meet(z, levels):
    beside = jnp.minimum(z, 1) + jnp.minimum(levels - 1 - z, 1)
    pl.semaphore_wait(pltpu.get_barrier_semaphore(), 3 + beside)


def start_send(src, dst, send_sem, recv_sem, device):
    copy = pltpu.make_async_remote_copy(
        src_ref=src,
        dst_ref=dst,
        send_sem=send_sem,
        recv_sem=recv_sem,
        device_id=device,
        device_id_type=MESH,
    )
    copy.start()
    return copy


def attend_kernel(
    levels, heads, group, parts, q_ref, k_ref, v_ref, pos_ref, resid_ref, weight_ref, stream_ref,
    weight, k_in, v_in, stacked, top, total, mixed, attended, projected, core_in, kept, from_y,
    ws, zs, zr, xs, xr, cs, cr, ys, yr,
):
    f32, bf16 = jnp.float32, jnp.bfloat16
    rows_per_load = weight.shape[0] // parts
    loads = []
    for part in range(parts):
        rows = slice(part * rows_per_load, (part + 1) * rows_per_load)
        loads.append(pltpu.make_async_copy(weight_ref.at[rows], weight.at[rows], ws.at[part]))
        loads[part].start()
    z, x, y, c = place_of()
    x_peer, y_peer, c_peer = at(z, 1 - x, y, c), at(z, x, 1 - y, c), at(z, x, y, 1 - c)
    announce(z, x, y, c, levels)
    meet(z, levels)
    own, incoming = (k_ref, v_ref), (k_in, v_in)
    z_sides = ((1, z < levels - 1), (-1, z > 0))
    mine = z * 2 + x

    def z_copy(i, side, k, first=False):
        ref = incoming[i].at[k * 2 + x]
        return pltpu.make_async_remote_copy(
            src_ref=own[i] if first else ref,
            dst_ref=ref,
            send_sem=zs.at[i, side, k],
            recv_sem=zr.at[i, k],
            device_id=at(z + z_sides[side][0], x, y, c),
            device_id_type=MESH,
        )

    def x_copy(i, k, first=False):
        ref = incoming[i].at[k * 2 + x]
        return pltpu.make_async_remote_copy(
            src_ref=own[i] if first else ref,
            dst_ref=ref,
            send_sem=xs.at[i, k],
            recv_sem=xr.at[i, k],
            device_id=x_peer,
            device_id_type=MESH,
        )

    def from_peer(i, k):
        ref = incoming[i].at[k * 2 + 1 - x]
        return pltpu.make_async_remote_copy(
            src_ref=ref,
            dst_ref=ref,
            send_sem=xs.at[i, k],
            recv_sem=xr.at[i, k],
            device_id=x_peer,
            device_id_type=MESH,
        )

    for i in range(2):
        for side, (_, there) in enumerate(z_sides):

            @pl.when(there)
            def _():
                z_copy(i, side, z, True).start()

        x_copy(i, z, True).start()

    rows = q_ref.shape[0]
    size = q_ref.shape[1] // (heads * group)
    for h in range(heads):
        for g in range(group):
            head = h * group + g
            stacked[h, g * rows : (g + 1) * rows, :] = q_ref[:, head * size : (head + 1) * size]
    query_pos = jnp.broadcast_to(pos_ref[mine], (rows, rows)).T
    scale = 1.0 / math.sqrt(size)

    def attend(keys, values, index, first=False):
        allowed = (pos_ref[index] <= query_pos)[None]

        def one(h, carry):
            columns = pl.ds(pl.multiple_of(h * size, size), size)
            scores = lax.dot_general(
                stacked[h], keys[:, columns], (((1,), (1,)), ((), ())), preferred_element_type=f32
            ).reshape(group, rows, rows)
            scores = jnp.where(allowed, scores * scale, -1e30)
            new_top = jnp.max(scores, axis=-1, keepdims=True)
            if not first:
                new_top = jnp.maximum(top[h], new_top)
            weights = jnp.where(allowed, jnp.exp(scores - new_top), 0.0)
            new_total = jnp.sum(weights, axis=-1, keepdims=True)
            update = jnp.dot(
                weights.astype(bf16).reshape(group * rows, rows),
                values[:, columns],
                preferred_element_type=f32,
            ).reshape(group, rows, size)
            if not first:
                fade = jnp.exp(top[h] - new_top)
                new_total = new_total + fade * total[h]
                update = update + fade * mixed[h]
            top[h] = new_top
            total[h] = new_total
            mixed[h] = update
            return carry

        lax.fori_loop(0, heads, one, 0)

    attend(k_ref, v_ref, mine, True)
    for turn in range(1, levels + 1):
        if turn < levels:
            k = level_at(z, turn, levels)
            for i in range(2):
                z_copy(i, 0, k).wait_recv()
                for side, (step, there) in enumerate(z_sides):

                    @pl.when(jnp.logical_and(there, (z - k) * step > 0))
                    def _():
                        z_copy(i, side, k).start()

                x_copy(i, k).start()
        last = level_at(z, turn - 1, levels)
        for i in range(2):
            from_peer(i, last).wait_recv()
        index = last * 2 + 1 - x
        attend(k_in.at[index], v_in.at[index], index)
        if turn < levels:
            attend(k_in.at[k * 2 + x], v_in.at[k * 2 + x], k * 2 + x)

    for h in range(heads):
        result = (mixed[h] / total[h]).astype(bf16)
        for g in range(group):
            head = h * group + g
            attended[:, head * size : (head + 1) * size] = result[g]
    for load in loads:
        load.wait()

    width = weight.shape[1] // parts
    sub = resid_ref.shape[0]
    c_copies, y_copies = [], []

    def cut(part):
        return slice(part * width, (part + 1) * width)

    def pass_on(part):
        c_copies[part].wait_recv()
        kept[part] = (
            projected[part, 1 - y, c].astype(f32) + core_in[part, 1 - y].astype(f32)
        ).astype(bf16)
        y_copies.append(
            start_send(kept.at[part], from_y.at[part], ys.at[part], yr.at[part], y_peer)
        )

    for part in range(parts):
        projected[part] = (
            jnp.dot(attended[...], weight[:, cut(part)], preferred_element_type=f32)
            .astype(bf16)
            .reshape(2, 2, sub, width)
        )
        c_copies.append(
            start_send(
                projected.at[part, :, 1 - c], core_in.at[part], cs.at[part], cr.at[part], c_peer
            )
        )
        if part:
            pass_on(part - 1)
    pass_on(parts - 1)
    for part in range(parts):
        own_sum = projected[part, y, c].astype(f32) + core_in[part, y].astype(f32)
        own_sum = own_sum + resid_ref[:, cut(part)].astype(f32)
        y_copies[part].wait_recv()
        stream_ref[:, cut(part)] = (own_sum + from_y[part].astype(f32)).astype(bf16)
    for copy in c_copies + y_copies:
        copy.wait_send()
    for i in range(2):
        for k in range(levels):
            x_copy(i, k).wait_send()
            for side, (step, there) in enumerate(z_sides):

                @pl.when(jnp.logical_and(there, (z - k) * step >= 0))
                def _():
                    z_copy(i, side, k).wait_send()


def attend(queries, keys, values, positions, resid_in, out_weight, levels):
    rows, width = keys.shape
    sub, model = resid_in.shape
    heads = width // HEAD_SIZE
    group = queries.shape[1] // width
    parts = 4
    vmem = pl.BlockSpec(memory_space=pltpu.VMEM)
    dma = pltpu.SemaphoreType.DMA
    f32, bf16 = jnp.float32, jnp.bfloat16
    return pl.pallas_call(
        functools.partial(attend_kernel, levels, heads, group, parts),
        out_shape=jax.ShapeDtypeStruct((sub, model), bf16),
        in_specs=[vmem] * 5 + [pl.BlockSpec(memory_space=pl.ANY)],
        out_specs=vmem,
        scratch_shapes=[
            pltpu.VMEM(out_weight.shape, bf16),
            pltpu.VMEM((levels * 2, rows, width), bf16),
            pltpu.VMEM((levels * 2, rows, width), bf16),
            pltpu.VMEM((heads, group * rows, HEAD_SIZE), bf16),
            pltpu.VMEM((heads, group, rows, 1), f32),
            pltpu.VMEM((heads, group, rows, 1), f32),
            pltpu.VMEM((heads, group, rows, HEAD_SIZE), f32),
            pltpu.VMEM(queries.shape, bf16),
            pltpu.VMEM((parts, 2, 2, sub, model // parts), bf16),
            pltpu.VMEM((parts, 2, sub, model // parts), bf16),
            pltpu.VMEM((parts, sub, model // parts), bf16),
            pltpu.VMEM((parts, sub, model // parts), bf16),
            dma((parts,)),
            dma((2, 2, levels)),
            dma((2, levels)),
            dma((2, levels)),
            dma((2, levels)),
        ]
        + [dma((parts,))] * 4,
        compiler_params=pltpu.CompilerParams(
            collective_id=0, has_side_effects=True, vmem_limit_bytes=VMEM_BYTES
        ),
    )(queries, keys, values, positions, resid_in, out_weight)


def stream_kernel(
    levels, sub, model, half, experts, slots, tile, stream_ref, gain_ref, router_ref,
    ids_ref, gate_ref, up_ref, hidden_ref, placing_ref, weight_ref,
    out_ref, gate_w, up_w, rows_ref, zs, zr, xs, xr, ys, yr, ds, dr, es, er, cs, cr, gs, us,
):
    loads = []
    for part in range(model // LOAD_ROWS):
        rows = slice(part * LOAD_ROWS, (part + 1) * LOAD_ROWS)
        loads.append(pltpu.make_async_copy(gate_ref.at[0, rows], gate_w.at[rows], gs.at[part]))
        loads.append(pltpu.make_async_copy(up_ref.at[0, rows], up_w.at[rows], us.at[part]))
    for load in loads:
        load.start()
    z, x, y, c = place_of()
    x_peer, y_peer, c_peer = at(z, 1 - x, y, c), at(z, x, 1 - y, c), at(z, x, y, 1 - c)
    announce(z, x, y, c, levels)

    stream = stream_ref[...]
    wide = stream.astype(jnp.float32)
    mean_square = jnp.mean(wide * wide, axis=-1, keepdims=True)
    normed = (wide * lax.rsqrt(mean_square + 1e-05) * gain_ref[...]).astype(jnp.bfloat16)

    normed_wide = normed.astype(jnp.float32)
    logits = [
        jnp.sum(normed_wide * router_ref[e : e + 1, :], axis=-1, keepdims=True)
        for e in range(experts)
    ]
    token = lax.broadcasted_iota(jnp.int32, (sub, sub), 0)
    same = token == lax.broadcasted_iota(jnp.int32, (sub, sub), 1)
    id0, id1 = (
        jnp.sum(
            jnp.where(same, ids_ref[i : i + 1, :].astype(jnp.float32), 0.0), axis=1, keepdims=True
        ).astype(jnp.int32)
        for i in range(2)
    )
    zero = jnp.zeros_like(logits[0])
    pick0, pick1 = zero, zero
    for e in range(experts):
        pick0 = pick0 + jnp.where(id0 == e, logits[e], 0.0)
        pick1 = pick1 + jnp.where(id1 == e, logits[e], 0.0)
    top = jnp.maximum(pick0, pick1)
    exp0, exp1 = jnp.exp(pick0 - top), jnp.exp(pick1 - top)
    gate0, gate1 = exp0 / (exp0 + exp1), exp1 / (exp0 + exp1)
    lane = lax.broadcasted_iota(jnp.int32, (sub, 128), 1)
    expert = lane % experts
    routed = jnp.logical_or(expert == id0, expert == id1)
    weight = jnp.where(expert == id0, gate0, 0.0) + jnp.where(expert == id1, gate1, 0.0)
    high = weight.astype(jnp.bfloat16).astype(jnp.float32)
    group = lane // experts
    tail = jnp.where(
        group == 0,
        jnp.where(routed, 1.0, 0.0),
        jnp.where(group == 1, high, jnp.where(group == 2, weight - high, 0.0)),
    )

    def block(k, bx, by):
        return ((k * 2 + bx) * 2 + by) * 2 + c

    mine = block(z, x, y)
    out_ref[mine, :, 0:model] = normed
    out_ref[mine, :, model : model + 128] = tail.astype(jnp.bfloat16)

    left, right = slice(0, half), slice(half, model + 128)
    pieces = (left, right)
    z_sides = ((1, z < levels - 1), (-1, z > 0))

    def z_copy(side, k, p):
        ref = out_ref.at[block(k, x, y), :, pieces[p]]
        return pltpu.make_async_remote_copy(
            src_ref=ref,
            dst_ref=ref,
            send_sem=zs.at[side, p, k],
            recv_sem=zr.at[p, k],
            device_id=at(z + z_sides[side][0], x, y, c),
            device_id_type=MESH,
        )

    def z_pass(k, p, whole=False):
        for side, (step, there) in enumerate(z_sides):
            behind = (z - k) * step

            @pl.when(jnp.logical_and(there, behind >= 0 if whole else behind > 0))
            def _():
                z_copy(side, k, p).start()

    meet(z, levels)
    for p in range(2):
        z_pass(z, p, True)
    at_end = z % (levels - 1) == 0
    x_copies, y_copies, d_copies, e_copies, c_copies = [], [], [], [], []

    def to_core(index):
        n = len(c_copies)
        ref = out_ref.at[index]
        c_copies.append(start_send(ref, ref, cs.at[n], cr.at[n], c_peer))
        return n

    sent = {d: [] for d in range(levels)}

    def finish(d):
        k = level_at(z, d, levels)
        d_copies[d].wait_recv()
        e_copies[d].wait_recv()
        sent[d].append(to_core(block(k, 1 - x, 1 - y)))

    mine_expert = lax.axis_index("exp")
    count = 8 * sub

    def experts_of(d):
        k = level_at(z, d, levels)
        for n in sent[d]:
            c_copies[n].wait_recv()
        info = out_ref[pl.ds(k * 8, 8), :, model : model + 128].reshape(count, 128)
        above = lax.broadcasted_iota(jnp.int32, (count, count), 0)
        below = lax.broadcasted_iota(jnp.int32, (count, count), 1)
        within = jnp.logical_and(above // sub == below // sub, below <= above)
        seen = jnp.dot(
            jnp.where(within, 1.0, 0.0).astype(jnp.bfloat16),
            info,
            preferred_element_type=jnp.float32,
        )
        wide_info = info.astype(jnp.float32)
        at_lane = lax.broadcasted_iota(jnp.int32, (count, 128), 1)

        def lane_sum(value, keep):
            return jnp.sum(jnp.where(keep, value, 0.0), axis=1, keepdims=True)

        is_mine = at_lane == mine_expert
        here = lane_sum(wide_info, is_mine)
        rank = lane_sum(seen, is_mine).astype(jnp.int32) - 1
        token_weight = lane_sum(
            wide_info,
            jnp.logical_or(at_lane == experts + mine_expert, at_lane == 2 * experts + mine_expert),
        )
        token = lax.broadcasted_iota(jnp.int32, (count, 1), 0)
        slot = jnp.where(here > 0.5, token // sub * slots + rank, -1)
        at_slot = lax.broadcasted_iota(jnp.int32, (count, 8 * slots), 1)
        placing = jnp.where(at_slot == slot, 1.0, 0.0).astype(jnp.bfloat16)
        placing_ref[k] = placing
        weight_ref[k] = jnp.broadcast_to(token_weight, (count, 128))
        picked_rows = jnp.where(at_slot == slot, 1.0, 0.0).T.astype(jnp.bfloat16)

        def pick(j, carry):
            columns = pl.ds(pl.multiple_of(j * 1024, 1024), 1024)
            block_in = out_ref[pl.ds(k * 8, 8), :, columns].reshape(count, 1024)
            rows_ref[:, columns] = jnp.dot(
                picked_rows, block_in, preferred_element_type=jnp.float32
            ).astype(jnp.bfloat16)
            return carry

        lax.fori_loop(0, model // 1024, pick, 0)
        if d == 0:
            for load in loads:
                load.wait()

        def unit(j, carry):
            columns = pl.ds(pl.multiple_of(j * tile, tile), tile)
            rows = rows_ref[...]
            gate = jnp.dot(rows, gate_w[:, columns], preferred_element_type=jnp.float32)
            up = jnp.dot(rows, up_w[:, columns], preferred_element_type=jnp.float32)
            hidden_ref[k, :, columns] = (gate * jax.nn.sigmoid(gate) * up).astype(jnp.bfloat16)
            return carry

        lax.fori_loop(0, hidden_ref.shape[2] // tile, unit, 0)

    for turn in range(levels + 1):
        near = level_at(z, turn - 1, levels) if turn else None
        far = level_at(z, turn, levels) if turn < levels else None
        for p in range(2):
            if turn < levels:
                if 0 < turn < levels - 1:
                    z_copy(0, far, p).wait_recv()
                    z_pass(far, p)
                elif turn:

                    @pl.when(at_end)
                    def _():
                        z_copy(0, far, p).wait_recv()

                n = turn * 2 + p
                ref = out_ref.at[block(far, x, y), :, pieces[p]]
                x_copies.append(start_send(ref, ref, xs.at[n], xr.at[n], x_peer))
                y_copies.append(start_send(ref, ref, ys.at[n], yr.at[n], y_peer))
            if turn:
                d = turn - 1
                if p == 0:
                    x_copies[d * 2].wait_recv()
                    ref = out_ref.at[block(near, 1 - x, y), :, left]
                    d_copies.append(start_send(ref, ref, ds.at[d], dr.at[d], y_peer))
                else:
                    y_copies[d * 2 + 1].wait_recv()
                    ref = out_ref.at[block(near, x, 1 - y), :, right]
                    e_copies.append(start_send(ref, ref, es.at[d], er.at[d], x_peer))
        if turn < levels:
            sent[turn].append(to_core(block(far, x, y)))
        if turn:
            x_copies[d * 2 + 1].wait_recv()
            sent[d].append(to_core(block(near, 1 - x, y)))
            y_copies[d * 2].wait_recv()
            sent[d].append(to_core(block(near, x, 1 - y)))
        if turn >= 2:
            finish(turn - 2)
            if turn == levels - 2:
                ahead = level_at(z, levels - 1, levels)

                @pl.when(jnp.logical_not(at_end))
                def _():
                    for p in range(2):
                        z_copy(0, ahead, p).wait_recv()
                        z_pass(ahead, p)

            experts_of(turn - 2)
    finish(levels - 1)
    experts_of(levels - 1)
    for copy in x_copies + y_copies + d_copies + e_copies + c_copies:
        copy.wait_send()
    for k in range(levels):
        for side, (step, there) in enumerate(z_sides):

            @pl.when(jnp.logical_and(there, (z - k) * step >= 0))
            def _():
                for p in range(2):
                    z_copy(side, k, p).wait_send()


def hidden_units(stream, norm_gain, router, expert_ids, gate, up, levels):
    sub, model = stream.shape
    experts = router.shape[1]
    width = gate.shape[2]
    slots = sub * expert_ids.shape[1] // experts
    vmem = pl.BlockSpec(memory_space=pltpu.VMEM)
    hbm = pl.BlockSpec(memory_space=pl.ANY)
    dma = pltpu.SemaphoreType.DMA
    bf16 = jnp.bfloat16
    return pl.pallas_call(
        functools.partial(
            stream_kernel, levels, sub, model, model // 2, experts, slots, width // 2
        ),
        out_shape=(
            jax.ShapeDtypeStruct((levels, 8 * slots, width), bf16),
            jax.ShapeDtypeStruct((levels, 8 * sub, 8 * slots), bf16),
            jax.ShapeDtypeStruct((levels, 8 * sub, 128), jnp.float32),
        ),
        in_specs=[vmem] * 4 + [hbm] * 2,
        out_specs=(vmem,) * 3,
        scratch_shapes=[
            pltpu.VMEM((levels * 8, sub, model + 128), bf16),
            pltpu.VMEM((model, width), bf16),
            pltpu.VMEM((model, width), bf16),
            pltpu.VMEM((8 * slots, model), bf16),
        ]
        + [dma((2, 2, levels)), dma((2, levels))]
        + [dma((levels * 2,))] * 4
        + [dma((levels,))] * 4
        + [dma((levels * 4,))] * 2
        + [dma((model // LOAD_ROWS,))] * 2,
        compiler_params=pltpu.CompilerParams(
            collective_id=1, has_side_effects=True, vmem_limit_bytes=VMEM_BYTES
        ),
    )(
        stream,
        norm_gain.reshape(1, model),
        router.T,
        expert_ids.T,
        gate,
        up,
    )


def sum_kernel(
    levels, sub, model, half, tile, hidden_ref, placing_ref, weight_ref, down_ref, stream_ref,
    out_ref, part_ref, down_w, core_in, first_in, second_in, z_in, total,
    corner_in, cs, cr, fs, fr, ss, sr, ps, zs, zr, pr, ls,
):
    def load(columns, n):
        return pltpu.make_async_copy(down_ref.at[0, :, columns], down_w.at[:, columns], ls.at[n])

    for n in range(model // tile):
        load(slice(n * tile, (n + 1) * tile), n).start()
    z, x, y, c = place_of()
    x_peer, y_peer, c_peer = at(z, 1 - x, y, c), at(z, x, 1 - y, c), at(z, x, y, 1 - c)
    announce(z, x, y, c, levels)
    f32, bf16 = jnp.float32, jnp.bfloat16
    units = levels * 2
    z_sides = ((1, z > 0), (-1, z < levels - 1))
    c_copies, stage2, stage3 = {}, {}, {}

    def place(u):
        return level_at(z, levels - 1 - u // 2, levels), u // 2, u % 2

    def terms_of(u):
        k, r, h = place(u)
        weight = jnp.concatenate([weight_ref[k]] * (tile // 128), axis=1)
        hidden = hidden_ref[k]
        placing = placing_ref[k]

        def one(j, carry):
            columns = pl.ds(pl.multiple_of(h * half + j * tile, tile), tile)
            if r == 0:
                load(columns, h * (half // tile) + j).wait()
            rows = jnp.dot(hidden, down_w[:, columns], preferred_element_type=f32).astype(bf16)
            spread = jnp.dot(placing, rows, preferred_element_type=f32)
            inner = pl.ds(pl.multiple_of(j * tile, tile), tile)
            part_ref[k, h, :, :, :, :, inner] = (
                (spread * weight).astype(bf16).reshape(2, 2, 2, sub, tile)
            )
            return carry

        lax.fori_loop(0, half // tile, one, 0)
        if u == 0:
            meet(z, levels)
        c_copies[u] = start_send(
            part_ref.at[k, h, :, :, 1 - c], core_in.at[r, h], cs.at[u], cr.at[u], c_peer
        )

    direct = {}
    inside = jnp.minimum(z * (levels - 1 - z), 1)

    def corner_copy(u, side, slot):
        k, _, h = place(u)
        if slot is None:
            slot = side * inside + 2 * (1 - inside)
        return pltpu.make_async_remote_copy(
            src_ref=part_ref.at[k, h, 1 - x, 1 - y, c],
            dst_ref=corner_in.at[slot, h],
            send_sem=ps.at[u],
            recv_sem=pr.at[slot, h],
            device_id=at(z + z_sides[side][0], x, y, c),
            device_id_type=MESH,
        )

    def corner_add(u, slot):
        k, _, h = place(u)
        corner_copy(u, 0, slot).wait_recv()
        part_ref[k, h, 1 - x, 1 - y, c] = (
            part_ref[k, h, 1 - x, 1 - y, c].astype(f32) + corner_in[slot, h].astype(f32)
        ).astype(bf16)

    def first_of(u):
        k, r, h = place(u)
        c_copies[u].wait_recv()
        for bx in range(2):
            for by in range(2):
                part_ref[k, h, bx, by, c] = (
                    part_ref[k, h, bx, by, c].astype(f32) + core_in[r, h, bx, by].astype(f32)
                ).astype(bf16)
        if r == levels - 1:
            for side, (_, outer) in enumerate(z_sides):
                pl.when(outer)(functools.partial(corner_add, u, side))
        elif r:
            if r == levels - 2:
                pl.when(inside == 1)(functools.partial(corner_add, u, 2))
            for side, (step, _) in enumerate(z_sides):

                @pl.when((k - z) * step > 0)
                def _():
                    corner_copy(u, side, side if r == levels - 2 else None).start()

            direct[u] = (
                start_send(
                    part_ref.at[k, h, 1 - x, y, c], first_in.at[r, h, 0],
                    fs.at[u], fr.at[u], x_peer,
                ),
                start_send(
                    part_ref.at[k, h, x, 1 - y, c], first_in.at[r, h, 1],
                    ss.at[u], sr.at[u], y_peer,
                ),
            )
            return
        if h:
            src, peer = part_ref.at[k, h, 1 - x, :, c], x_peer
        else:
            src, peer = part_ref.at[k, h, :, 1 - y, c], y_peer
        stage2[u] = start_send(src, first_in.at[r, h], fs.at[u], fr.at[u], peer)

    def second_of(u):
        k, r, h = place(u)
        if u not in stage2:
            return
        stage2[u].wait_recv()
        bx, by, other, peer = (x, 1 - y, 1 - y, y_peer) if h else (1 - x, y, 1 - x, x_peer)
        part_ref[k, h, bx, by, c] = (
            part_ref[k, h, bx, by, c].astype(f32) + first_in[r, h, other].astype(f32)
        ).astype(bf16)
        stage3[u] = start_send(
            part_ref.at[k, h, bx, by, c], second_in.at[r, h], ss.at[u], sr.at[u], peer
        )

    def z_copy(u, side):
        k, _, h = place(u)
        return pltpu.make_async_remote_copy(
            src_ref=part_ref.at[k, h, x, y, c],
            dst_ref=z_in.at[side, k, h],
            send_sem=zs.at[u],
            recv_sem=zr.at[side, k, h],
            device_id=at(z + z_sides[side][0], x, y, c),
            device_id_type=MESH,
        )

    def z_send(u, with_outer):
        k, _, h = place(u)
        for side, (step, outer) in enumerate(z_sides):
            right_way = (k - z) * step > 0

            @pl.when(jnp.logical_and(right_way, outer if with_outer else jnp.logical_not(outer)))
            def _():
                if with_outer:
                    z_copy(u, side).wait_recv()
                    part_ref[k, h, x, y, c] = (
                        part_ref[k, h, x, y, c].astype(f32) + z_in[side, k, h].astype(f32)
                    ).astype(bf16)
                z_copy(u, side).start()

    def third_of(u):
        k, r, h = place(u)
        value = part_ref[k, h, x, y, c].astype(f32)
        if u in direct:
            for i, copy in enumerate(direct[u]):
                copy.wait_recv()
                value = value + first_in[r, h, i].astype(f32)
        else:
            stage3[u].wait_recv()
            value = value + first_in[r, h, y if h else x].astype(f32)
            value = value + second_in[r, h].astype(f32)
        if r < levels - 1:
            part_ref[k, h, x, y, c] = value.astype(bf16)
            z_send(u, False)
        else:
            total[h] = stream_ref[:, h * half : (h + 1) * half].astype(f32) + value

    second_lag, direct_lag, third_lag = 2, 3, 5
    terms_of(0)
    for step in range(units + third_lag):
        if step < units:
            first_of(step)
        if step + 1 < units:
            terms_of(step + 1)
        if 0 <= step - second_lag < units:
            second_of(step - second_lag)
        for u in range(units):
            outer = 0 < u // 2 < levels - 1
            lag = direct_lag if outer else third_lag
            if step == u + lag:
                third_of(u)
            if u < units - 2 and step == u + lag + (2, 4, 0)[u // 2]:
                z_send(u, True)
    for u in range(units - 2, units):
        h = u % 2
        for side, (_, outer) in enumerate(z_sides):

            @pl.when(outer)
            def _():
                z_copy(u, side).wait_recv()
                total[h] += z_in[side, z, h].astype(f32)

        out_ref[:, h * half : (h + 1) * half] = total[h].astype(bf16)
    for u in range(units):
        c_copies[u].wait_send()
        for copy in direct[u] if u in direct else (stage2[u], stage3[u]):
            copy.wait_send()
        if u in direct:
            corner_copy(u, 0, 0).wait_send()
        if u < units - 2:
            z_copy(u, 0).wait_send()


def sum_terms(hidden, placing, weight, down, stream, levels):
    sub, model = stream.shape
    half = model // 2
    tile = 1024
    vmem = pl.BlockSpec(memory_space=pltpu.VMEM)
    dma = pltpu.SemaphoreType.DMA
    bf16 = jnp.bfloat16
    return pl.pallas_call(
        functools.partial(sum_kernel, levels, sub, model, half, tile),
        out_shape=jax.ShapeDtypeStruct((sub, model), bf16),
        in_specs=[vmem] * 3 + [pl.BlockSpec(memory_space=pl.ANY), vmem],
        out_specs=vmem,
        scratch_shapes=[
            pltpu.VMEM((levels, 2, 2, 2, 2, sub, half), bf16),
            pltpu.VMEM(down.shape[1:], bf16),
            pltpu.VMEM((levels, 2, 2, 2, sub, half), bf16),
            pltpu.VMEM((levels, 2, 2, sub, half), bf16),
            pltpu.VMEM((levels, 2, sub, half), bf16),
            pltpu.VMEM((2, levels, 2, sub, half), bf16),
            pltpu.VMEM((2, sub, half), jnp.float32),
            pltpu.VMEM((3, 2, sub, half), bf16),
        ]
        + [dma((levels * 2,))] * 8
        + [dma((2, levels, 2)), dma((3, 2)), dma((model // tile,))],
        compiler_params=pltpu.CompilerParams(
            collective_id=2, has_side_effects=True, vmem_limit_bytes=VMEM_BYTES
        ),
    )(hidden, placing, weight, down, stream)


def on_device(
    levels,
    queries,
    keys,
    values,
    resid_in,
    span_order,
    out_weight,
    norm_gain,
    router,
    expert_ids,
    w_gate,
    w_up,
    w_down,
):
    blocks = levels * 2
    per_block = queries.shape[0] // SPAN
    within = jnp.arange(SPAN, dtype=jnp.int32)
    positions = span_order.reshape(blocks, 1, per_block, 1) * SPAN + within
    positions = positions.astype(jnp.float32).reshape(blocks, 1, per_block * SPAN)
    stream = attend(queries, keys, values, positions, resid_in, out_weight, levels)
    hidden, placing, weight = hidden_units(
        stream, norm_gain, router, expert_ids, w_gate, w_up, levels
    )
    return sum_terms(hidden, placing, weight, w_down, stream, levels)


def solution(mesh):
    placed = (
        P("ctx", "exp"),
        P("ctx", "exp"),
        P("ctx", "exp"),
        P(("ctx", "exp"), None),
        P(),
        P("exp", None),
        P(),
        P(),
        P(("ctx", "exp"), None),
        P("exp", None, "ctx"),
        P("exp", None, "ctx"),
        P("exp", "ctx", None),
    )
    levels = mesh.shape["ctx"] // 2

    def body(queries, keys, values, resid_in, *rest):
        blocks = resid_in.size * mesh.size * 2
        small = mesh.shape["exp"] == 4 and levels == 4 and blocks * 4 <= VMEM_BYTES
        local = functools.partial(on_device, levels) if small else on_device_xla
        return local(queries, keys, values, resid_in, *rest)

    return jax.shard_map(
        body, mesh=mesh, in_specs=placed, out_specs=P(("ctx", "exp"), None), check_vma=False
    )
```

```python
import functools
import math

import jax
import jax.numpy as jnp
from jax import lax
from jax.experimental import pallas as pl
from jax.experimental.pallas import tpu as pltpu
from jax.sharding import PartitionSpec as P

HEAD_SIZE = 128
SPAN = 64


def true_positions(row_ids, span_order):
    span_ids = jnp.arange(span_order.shape[0], dtype=jnp.int32)
    matches = (row_ids // SPAN)[:, None] == span_ids[None, :]
    return jnp.sum(jnp.where(matches, span_order[None, :], 0), axis=1) * SPAN + row_ids % SPAN


def on_device_xla(
    queries,
    keys,
    values,
    resid_in,
    span_order,
    out_weight,
    norm_gain,
    router,
    expert_ids,
    w_gate,
    w_up,
    w_down,
):
    tok_rows = queries.shape[0]
    kv_heads = keys.shape[1] // HEAD_SIZE
    head_cluster = queries.shape[1] // HEAD_SIZE // kv_heads
    ctx_index = lax.axis_index("ctx")
    query_pos = true_positions(
        ctx_index * tok_rows + jnp.arange(tok_rows, dtype=jnp.int32), span_order
    )
    shaped_queries = queries.reshape(tok_rows, kv_heads, head_cluster, HEAD_SIZE)
    score_scale = 1.0 / math.sqrt(HEAD_SIZE)
    pieces = (
        lax.all_gather(keys, "ctx", axis=0, tiled=True),
        lax.all_gather(values, "ctx", axis=0, tiled=True),
    )
    key_pos = true_positions(jnp.arange(pieces[0].shape[0], dtype=jnp.int32), span_order)
    running_max = jnp.full((kv_heads, head_cluster, tok_rows), -1e30, jnp.float32)
    key_block, value_block = pieces
    key_count = key_block.shape[0]
    key_head_rows = key_block.reshape(key_count, kv_heads, HEAD_SIZE)
    value_head_rows = value_block.reshape(key_count, kv_heads, HEAD_SIZE)
    scores = jnp.einsum(
        "qhgd,khd->hgqk", shaped_queries, key_head_rows, preferred_element_type=jnp.float32
    )
    allowed = key_pos[None, :] <= query_pos[:, None]
    scores = jnp.where(allowed[None, None], scores * score_scale, -1e30)
    new_max = jnp.maximum(running_max, jnp.max(scores, axis=-1))
    weights = jnp.where(allowed[None, None], jnp.exp(scores - new_max[..., None]), 0.0)
    running_sum = jnp.sum(weights, axis=-1)
    update = jnp.einsum(
        "hgqk,khd->qhgd",
        weights.astype(jnp.bfloat16),
        value_head_rows,
        preferred_element_type=jnp.float32,
    )
    weighted = update
    running_max, running_sum, weighted = (new_max, running_sum, weighted)
    attended = (
        (weighted / jnp.transpose(running_sum, (2, 0, 1))[..., None])
        .astype(jnp.bfloat16)
        .reshape(tok_rows, -1)
    )
    projected = jnp.dot(attended, out_weight, preferred_element_type=jnp.float32)
    own_sum = lax.psum_scatter(
        projected.astype(jnp.bfloat16), "exp", scatter_dimension=0, tiled=True
    ).astype(jnp.float32)
    stream = (resid_in.astype(jnp.float32) + own_sum).astype(jnp.bfloat16)
    stream_wide = stream.astype(jnp.float32)
    mean_square = jnp.mean(stream_wide * stream_wide, axis=-1, keepdims=True)
    normed = (stream_wide * lax.rsqrt(mean_square + 1e-05) * norm_gain).astype(jnp.bfloat16)
    model_dim = normed.shape[1]
    logits = jnp.dot(normed.astype(jnp.float32), router, precision=lax.Precision.HIGHEST)
    experts = router.shape[1]
    expert_axis = jnp.arange(experts, dtype=jnp.int32)
    picked = expert_ids[:, :, None] == expert_axis[None, None, :]
    chosen = jnp.sum(jnp.where(picked, logits[:, None, :], 0.0), axis=-1)
    mixing = jax.nn.softmax(chosen, axis=-1)
    token_weight = jnp.sum(jnp.where(picked, mixing[:, :, None], 0.0), axis=1)
    routed = jnp.any(picked, axis=1)
    rank_of = jnp.cumsum(routed.astype(jnp.int32), axis=0) - 1
    slot_count = resid_in.shape[0] * expert_ids.shape[1] // experts
    slot_axis = jnp.arange(slot_count, dtype=jnp.int32)
    placing = jnp.logical_and(
        routed.T[:, None, :], rank_of.T[:, None, :] == slot_axis[None, :, None]
    )
    outgoing = jnp.einsum(
        "est,td->esd", placing.astype(jnp.bfloat16), normed, preferred_element_type=jnp.float32
    ).astype(jnp.bfloat16)
    arrived = lax.all_to_all(outgoing, "exp", split_axis=0, concat_axis=0, tiled=True)
    rows_in = lax.all_gather(arrived.reshape(-1, model_dim), "ctx", axis=0, tiled=True)
    gate_part = jnp.dot(rows_in, w_gate[0], preferred_element_type=jnp.float32)
    up_part = jnp.dot(rows_in, w_up[0], preferred_element_type=jnp.float32)
    hidden = (jax.nn.silu(gate_part) * up_part).astype(jnp.bfloat16)
    partials = jnp.dot(hidden, w_down[0], preferred_element_type=jnp.float32)
    own_rows = lax.psum_scatter(
        partials.astype(jnp.bfloat16), "ctx", scatter_dimension=0, tiled=True
    )
    results = own_rows.reshape(experts, slot_count, model_dim)
    returned = lax.all_to_all(results, "exp", split_axis=0, concat_axis=0, tiled=True)
    coefficient = placing.astype(jnp.float32) * token_weight.T[:, None, :]
    combined = jnp.einsum("est,esd->td", coefficient, returned.astype(jnp.float32))
    return (stream_wide + combined).astype(jnp.bfloat16)


VMEM_BYTES = 60 * 2**20
LOAD_ROWS = 512
MESH = pl.DeviceIdType.MESH


def place_of():
    ctx, exp = lax.axis_index("ctx"), lax.axis_index("exp")
    return ctx // 2, ctx % 2, exp // 2, exp % 2


def at(z, x, y, c):
    return (z * 2 + x, y * 2 + c)


def level_at(z, turn, levels):
    upper = z // (levels // 2)
    sign = 1 - 2 * upper
    inner = z * (1 - upper) + (levels - 1 - z) * upper
    beyond = jnp.minimum(jnp.maximum(turn - 2 * inner, 0), 1)
    step = (turn + 1) // 2 * (1 if turn % 2 else -1)
    return z + sign * ((1 - beyond) * step + beyond * (turn - inner))


def neighbours(z, x, y, c, levels):
    return (
        (at(z, 1 - x, y, c), None),
        (at(z, x, 1 - y, c), None),
        (at(z, x, y, 1 - c), None),
        (at(z - 1, x, y, c), z > 0),
        (at(z + 1, x, y, c), z < levels - 1),
    )


def announce(z, x, y, c, levels):
    barrier = pltpu.get_barrier_semaphore()
    for device, there in neighbours(z, x, y, c, levels):

        def signal():
            pl.semaphore_signal(barrier, inc=1, device_id=device, device_id_type=MESH)

        if there is None:
            signal()
        else:
            pl.when(there)(signal)


def meet(z, levels):
    beside = jnp.minimum(z, 1) + jnp.minimum(levels - 1 - z, 1)
    pl.semaphore_wait(pltpu.get_barrier_semaphore(), 3 + beside)


def start_send(src, dst, send_sem, recv_sem, device):
    copy = pltpu.make_async_remote_copy(
        src_ref=src,
        dst_ref=dst,
        send_sem=send_sem,
        recv_sem=recv_sem,
        device_id=device,
        device_id_type=MESH,
    )
    copy.start()
    return copy


def attend_kernel(
    levels, heads, group, parts, q_ref, k_ref, v_ref, order_ref, resid_ref, weight_ref, stream_ref,
    weight, k_in, v_in, stacked, top, total, mixed, attended, projected, core_in, kept, from_y,
    ws, zs, zr, xs, xr, cs, cr, ys, yr,
):
    f32, bf16 = jnp.float32, jnp.bfloat16
    rows_per_load = weight.shape[0] // parts
    loads = []
    for part in range(parts):
        rows = slice(part * rows_per_load, (part + 1) * rows_per_load)
        loads.append(pltpu.make_async_copy(weight_ref.at[rows], weight.at[rows], ws.at[part]))
        loads[part].start()
    z, x, y, c = place_of()
    x_peer, y_peer, c_peer = at(z, 1 - x, y, c), at(z, x, 1 - y, c), at(z, x, y, 1 - c)
    announce(z, x, y, c, levels)
    meet(z, levels)
    own, incoming = (k_ref, v_ref), (k_in, v_in)
    z_sides = ((1, z < levels - 1), (-1, z > 0))
    mine = z * 2 + x

    def z_copy(i, side, k, first=False):
        ref = incoming[i].at[k * 2 + x]
        return pltpu.make_async_remote_copy(
            src_ref=own[i] if first else ref,
            dst_ref=ref,
            send_sem=zs.at[i, side, k],
            recv_sem=zr.at[i, k],
            device_id=at(z + z_sides[side][0], x, y, c),
            device_id_type=MESH,
        )

    def x_copy(i, k, first=False):
        ref = incoming[i].at[k * 2 + x]
        return pltpu.make_async_remote_copy(
            src_ref=own[i] if first else ref,
            dst_ref=ref,
            send_sem=xs.at[i, k],
            recv_sem=xr.at[i, k],
            device_id=x_peer,
            device_id_type=MESH,
        )

    def from_peer(i, k):
        ref = incoming[i].at[k * 2 + 1 - x]
        return pltpu.make_async_remote_copy(
            src_ref=ref,
            dst_ref=ref,
            send_sem=xs.at[i, k],
            recv_sem=xr.at[i, k],
            device_id=x_peer,
            device_id_type=MESH,
        )

    for i in range(2):
        for side, (_, there) in enumerate(z_sides):

            @pl.when(there)
            def _():
                z_copy(i, side, z, True).start()

        x_copy(i, z, True).start()

    rows = q_ref.shape[0]
    size = q_ref.shape[1] // (heads * group)
    for h in range(heads):
        for g in range(group):
            head = h * group + g
            stacked[h, g * rows : (g + 1) * rows, :] = q_ref[:, head * size : (head + 1) * size]
    lane = lax.broadcasted_iota(jnp.int32, (1, rows), 1)

    def positions(index):
        spans = rows // SPAN
        span = jnp.zeros((1, rows), jnp.int32)
        for n in range(spans):
            span = jnp.where(lane // SPAN == n, order_ref[index * spans + n], span)
        return (span * SPAN + lane % SPAN).astype(f32)

    query_pos = jnp.broadcast_to(positions(mine), (rows, rows)).T
    scale = 1.0 / math.sqrt(size)

    def attend(keys, values, index, first=False):
        allowed = (positions(index) <= query_pos)[None]

        def one(h, carry):
            columns = pl.ds(pl.multiple_of(h * size, size), size)
            scores = lax.dot_general(
                stacked[h], keys[:, columns], (((1,), (1,)), ((), ())), preferred_element_type=f32
            ).reshape(group, rows, rows)
            scores = jnp.where(allowed, scores * scale, -1e30)
            new_top = jnp.max(scores, axis=-1, keepdims=True)
            if not first:
                new_top = jnp.maximum(top[h], new_top)
            weights = jnp.where(allowed, jnp.exp(scores - new_top), 0.0)
            new_total = jnp.sum(weights, axis=-1, keepdims=True)
            update = jnp.dot(
                weights.astype(bf16).reshape(group * rows, rows),
                values[:, columns],
                preferred_element_type=f32,
            ).reshape(group, rows, size)
            if not first:
                fade = jnp.exp(top[h] - new_top)
                new_total = new_total + fade * total[h]
                update = update + fade * mixed[h]
            top[h] = new_top
            total[h] = new_total
            mixed[h] = update
            return carry

        lax.fori_loop(0, heads, one, 0)

    attend(k_ref, v_ref, mine, True)
    for turn in range(1, levels + 1):
        if turn < levels:
            k = level_at(z, turn, levels)
            for i in range(2):
                z_copy(i, 0, k).wait_recv()
                for side, (step, there) in enumerate(z_sides):

                    @pl.when(jnp.logical_and(there, (z - k) * step > 0))
                    def _():
                        z_copy(i, side, k).start()

                x_copy(i, k).start()
        last = level_at(z, turn - 1, levels)
        for i in range(2):
            from_peer(i, last).wait_recv()
        index = last * 2 + 1 - x
        attend(k_in.at[index], v_in.at[index], index)
        if turn < levels:
            attend(k_in.at[k * 2 + x], v_in.at[k * 2 + x], k * 2 + x)

    for h in range(heads):
        result = (mixed[h] / total[h]).astype(bf16)
        for g in range(group):
            head = h * group + g
            attended[:, head * size : (head + 1) * size] = result[g]
    for load in loads:
        load.wait()

    width = weight.shape[1] // parts
    sub = resid_ref.shape[0]
    c_copies, y_copies = [], []

    def cut(part):
        return slice(part * width, (part + 1) * width)

    def pass_on(part):
        c_copies[part].wait_recv()
        kept[part] = (
            projected[part, 1 - y, c].astype(f32) + core_in[part, 1 - y].astype(f32)
        ).astype(bf16)
        y_copies.append(
            start_send(kept.at[part], from_y.at[part], ys.at[part], yr.at[part], y_peer)
        )

    for part in range(parts):
        projected[part] = (
            jnp.dot(attended[...], weight[:, cut(part)], preferred_element_type=f32)
            .astype(bf16)
            .reshape(2, 2, sub, width)
        )
        c_copies.append(
            start_send(
                projected.at[part, :, 1 - c], core_in.at[part], cs.at[part], cr.at[part], c_peer
            )
        )
        if part:
            pass_on(part - 1)
    pass_on(parts - 1)
    for part in range(parts):
        own_sum = projected[part, y, c].astype(f32) + core_in[part, y].astype(f32)
        own_sum = own_sum + resid_ref[:, cut(part)].astype(f32)
        y_copies[part].wait_recv()
        stream_ref[:, cut(part)] = (own_sum + from_y[part].astype(f32)).astype(bf16)
    for copy in c_copies + y_copies:
        copy.wait_send()
    for i in range(2):
        for k in range(levels):
            x_copy(i, k).wait_send()
            for side, (step, there) in enumerate(z_sides):

                @pl.when(jnp.logical_and(there, (z - k) * step >= 0))
                def _():
                    z_copy(i, side, k).wait_send()


def attend(queries, keys, values, span_order, resid_in, out_weight, levels):
    rows, width = keys.shape
    sub, model = resid_in.shape
    heads = width // HEAD_SIZE
    group = queries.shape[1] // width
    parts = 4
    vmem = pl.BlockSpec(memory_space=pltpu.VMEM)
    dma = pltpu.SemaphoreType.DMA
    f32, bf16 = jnp.float32, jnp.bfloat16
    return pl.pallas_call(
        functools.partial(attend_kernel, levels, heads, group, parts),
        out_shape=jax.ShapeDtypeStruct((sub, model), bf16),
        in_specs=[vmem] * 3
        + [pl.BlockSpec(memory_space=pltpu.SMEM), vmem, pl.BlockSpec(memory_space=pl.ANY)],
        out_specs=vmem,
        scratch_shapes=[
            pltpu.VMEM(out_weight.shape, bf16),
            pltpu.VMEM((levels * 2, rows, width), bf16),
            pltpu.VMEM((levels * 2, rows, width), bf16),
            pltpu.VMEM((heads, group * rows, HEAD_SIZE), bf16),
            pltpu.VMEM((heads, group, rows, 1), f32),
            pltpu.VMEM((heads, group, rows, 1), f32),
            pltpu.VMEM((heads, group, rows, HEAD_SIZE), f32),
            pltpu.VMEM(queries.shape, bf16),
            pltpu.VMEM((parts, 2, 2, sub, model // parts), bf16),
            pltpu.VMEM((parts, 2, sub, model // parts), bf16),
            pltpu.VMEM((parts, sub, model // parts), bf16),
            pltpu.VMEM((parts, sub, model // parts), bf16),
            dma((parts,)),
            dma((2, 2, levels)),
            dma((2, levels)),
            dma((2, levels)),
            dma((2, levels)),
        ]
        + [dma((parts,))] * 4,
        compiler_params=pltpu.CompilerParams(
            collective_id=0, has_side_effects=True, vmem_limit_bytes=VMEM_BYTES
        ),
    )(queries, keys, values, span_order, resid_in, out_weight)


def stream_kernel(
    levels, sub, model, half, experts, slots, tile, stream_ref, gain_ref, router_ref,
    ids_ref, gate_ref, up_ref, hidden_ref, placing_ref, weight_ref,
    out_ref, gate_w, up_w, rows_ref, zs, zr, xs, xr, ys, yr, ds, dr, es, er, cs, cr, gs, us,
):
    loads = []
    for part in range(model // LOAD_ROWS):
        rows = slice(part * LOAD_ROWS, (part + 1) * LOAD_ROWS)
        loads.append(pltpu.make_async_copy(gate_ref.at[0, rows], gate_w.at[rows], gs.at[part]))
        loads.append(pltpu.make_async_copy(up_ref.at[0, rows], up_w.at[rows], us.at[part]))
    for load in loads:
        load.start()
    z, x, y, c = place_of()
    x_peer, y_peer, c_peer = at(z, 1 - x, y, c), at(z, x, 1 - y, c), at(z, x, y, 1 - c)
    announce(z, x, y, c, levels)

    stream = stream_ref[...]
    wide = stream.astype(jnp.float32)
    mean_square = jnp.mean(wide * wide, axis=-1, keepdims=True)
    normed = (wide * lax.rsqrt(mean_square + 1e-05) * gain_ref[...]).astype(jnp.bfloat16)

    normed_wide = normed.astype(jnp.float32)
    logits = [
        jnp.sum(normed_wide * router_ref[e : e + 1, :], axis=-1, keepdims=True)
        for e in range(experts)
    ]
    token = lax.broadcasted_iota(jnp.int32, (sub, sub), 0)
    same = token == lax.broadcasted_iota(jnp.int32, (sub, sub), 1)
    id0, id1 = (
        jnp.sum(
            jnp.where(same, ids_ref[i : i + 1, :].astype(jnp.float32), 0.0), axis=1, keepdims=True
        ).astype(jnp.int32)
        for i in range(2)
    )
    zero = jnp.zeros_like(logits[0])
    pick0, pick1 = zero, zero
    for e in range(experts):
        pick0 = pick0 + jnp.where(id0 == e, logits[e], 0.0)
        pick1 = pick1 + jnp.where(id1 == e, logits[e], 0.0)
    top = jnp.maximum(pick0, pick1)
    exp0, exp1 = jnp.exp(pick0 - top), jnp.exp(pick1 - top)
    gate0, gate1 = exp0 / (exp0 + exp1), exp1 / (exp0 + exp1)
    lane = lax.broadcasted_iota(jnp.int32, (sub, 128), 1)
    expert = lane % experts
    routed = jnp.logical_or(expert == id0, expert == id1)
    weight = jnp.where(expert == id0, gate0, 0.0) + jnp.where(expert == id1, gate1, 0.0)
    high = weight.astype(jnp.bfloat16).astype(jnp.float32)
    group = lane // experts
    tail = jnp.where(
        group == 0,
        jnp.where(routed, 1.0, 0.0),
        jnp.where(group == 1, high, jnp.where(group == 2, weight - high, 0.0)),
    )

    def block(k, bx, by):
        return ((k * 2 + bx) * 2 + by) * 2 + c

    mine = block(z, x, y)
    out_ref[mine, :, 0:model] = normed
    out_ref[mine, :, model : model + 128] = tail.astype(jnp.bfloat16)

    left, right = slice(0, half), slice(half, model + 128)
    pieces = (left, right)
    z_sides = ((1, z < levels - 1), (-1, z > 0))

    def z_copy(side, k, p):
        ref = out_ref.at[block(k, x, y), :, pieces[p]]
        return pltpu.make_async_remote_copy(
            src_ref=ref,
            dst_ref=ref,
            send_sem=zs.at[side, p, k],
            recv_sem=zr.at[p, k],
            device_id=at(z + z_sides[side][0], x, y, c),
            device_id_type=MESH,
        )

    def z_pass(k, p, whole=False):
        for side, (step, there) in enumerate(z_sides):
            behind = (z - k) * step

            @pl.when(jnp.logical_and(there, behind >= 0 if whole else behind > 0))
            def _():
                z_copy(side, k, p).start()

    meet(z, levels)
    for p in range(2):
        z_pass(z, p, True)
    at_end = z % (levels - 1) == 0
    x_copies, y_copies, d_copies, e_copies, c_copies = [], [], [], [], []

    def to_core(index):
        n = len(c_copies)
        ref = out_ref.at[index]
        c_copies.append(start_send(ref, ref, cs.at[n], cr.at[n], c_peer))
        return n

    sent = {d: [] for d in range(levels)}

    def finish(d):
        k = level_at(z, d, levels)
        d_copies[d].wait_recv()
        e_copies[d].wait_recv()
        sent[d].append(to_core(block(k, 1 - x, 1 - y)))

    mine_expert = lax.axis_index("exp")
    count = 8 * sub

    def experts_of(d):
        k = level_at(z, d, levels)
        for n in sent[d]:
            c_copies[n].wait_recv()
        info = out_ref[pl.ds(k * 8, 8), :, model : model + 128].reshape(count, 128)
        above = lax.broadcasted_iota(jnp.int32, (count, count), 0)
        below = lax.broadcasted_iota(jnp.int32, (count, count), 1)
        within = jnp.logical_and(above // sub == below // sub, below <= above)
        seen = jnp.dot(
            jnp.where(within, 1.0, 0.0).astype(jnp.bfloat16),
            info,
            preferred_element_type=jnp.float32,
        )
        wide_info = info.astype(jnp.float32)
        at_lane = lax.broadcasted_iota(jnp.int32, (count, 128), 1)

        def lane_sum(value, keep):
            return jnp.sum(jnp.where(keep, value, 0.0), axis=1, keepdims=True)

        is_mine = at_lane == mine_expert
        here = lane_sum(wide_info, is_mine)
        rank = lane_sum(seen, is_mine).astype(jnp.int32) - 1
        token_weight = lane_sum(
            wide_info,
            jnp.logical_or(at_lane == experts + mine_expert, at_lane == 2 * experts + mine_expert),
        )
        token = lax.broadcasted_iota(jnp.int32, (count, 1), 0)
        slot = jnp.where(here > 0.5, token // sub * slots + rank, -1)
        at_slot = lax.broadcasted_iota(jnp.int32, (count, 8 * slots), 1)
        placing = jnp.where(at_slot == slot, 1.0, 0.0).astype(jnp.bfloat16)
        placing_ref[k] = placing
        weight_ref[k] = jnp.broadcast_to(token_weight, (count, 128))
        picked_rows = jnp.where(at_slot == slot, 1.0, 0.0).T.astype(jnp.bfloat16)

        def pick(j, carry):
            columns = pl.ds(pl.multiple_of(j * 1024, 1024), 1024)
            block_in = out_ref[pl.ds(k * 8, 8), :, columns].reshape(count, 1024)
            rows_ref[:, columns] = jnp.dot(
                picked_rows, block_in, preferred_element_type=jnp.float32
            ).astype(jnp.bfloat16)
            return carry

        lax.fori_loop(0, model // 1024, pick, 0)
        if d == 0:
            for load in loads:
                load.wait()

        for columns in (slice(0, tile), slice(tile, hidden_ref.shape[2])):
            rows = rows_ref[...]
            gate = jnp.dot(rows, gate_w[:, columns], preferred_element_type=jnp.float32)
            up = jnp.dot(rows, up_w[:, columns], preferred_element_type=jnp.float32)
            hidden_ref[k, :, columns] = (gate * jax.nn.sigmoid(gate) * up).astype(jnp.bfloat16)

    for turn in range(levels + 1):
        near = level_at(z, turn - 1, levels) if turn else None
        far = level_at(z, turn, levels) if turn < levels else None
        for p in range(2):
            if turn < levels:
                if 0 < turn < levels - 1:
                    z_copy(0, far, p).wait_recv()
                    z_pass(far, p)
                elif turn:

                    @pl.when(at_end)
                    def _():
                        z_copy(0, far, p).wait_recv()

                n = turn * 2 + p
                ref = out_ref.at[block(far, x, y), :, pieces[p]]
                x_copies.append(start_send(ref, ref, xs.at[n], xr.at[n], x_peer))
                y_copies.append(start_send(ref, ref, ys.at[n], yr.at[n], y_peer))
            if turn:
                d = turn - 1
                if p == 0:
                    x_copies[d * 2].wait_recv()
                    ref = out_ref.at[block(near, 1 - x, y), :, left]
                    d_copies.append(start_send(ref, ref, ds.at[d], dr.at[d], y_peer))
                else:
                    y_copies[d * 2 + 1].wait_recv()
                    ref = out_ref.at[block(near, x, 1 - y), :, right]
                    e_copies.append(start_send(ref, ref, es.at[d], er.at[d], x_peer))
        if turn < levels:
            sent[turn].append(to_core(block(far, x, y)))
        if turn:
            x_copies[d * 2 + 1].wait_recv()
            sent[d].append(to_core(block(near, 1 - x, y)))
            y_copies[d * 2].wait_recv()
            sent[d].append(to_core(block(near, x, 1 - y)))
        if turn >= 2:
            finish(turn - 2)
            if turn == levels - 2:
                ahead = level_at(z, levels - 1, levels)

                @pl.when(jnp.logical_not(at_end))
                def _():
                    for p in range(2):
                        z_copy(0, ahead, p).wait_recv()
                        z_pass(ahead, p)

            experts_of(turn - 2)
    finish(levels - 1)
    experts_of(levels - 1)
    for copy in x_copies + y_copies + d_copies + e_copies + c_copies:
        copy.wait_send()
    for k in range(levels):
        for side, (step, there) in enumerate(z_sides):

            @pl.when(jnp.logical_and(there, (z - k) * step >= 0))
            def _():
                for p in range(2):
                    z_copy(side, k, p).wait_send()


def hidden_units(stream, norm_gain, router, expert_ids, gate, up, levels):
    sub, model = stream.shape
    experts = router.shape[1]
    width = gate.shape[2]
    slots = sub * expert_ids.shape[1] // experts
    vmem = pl.BlockSpec(memory_space=pltpu.VMEM)
    hbm = pl.BlockSpec(memory_space=pl.ANY)
    dma = pltpu.SemaphoreType.DMA
    bf16 = jnp.bfloat16
    return pl.pallas_call(
        functools.partial(
            stream_kernel, levels, sub, model, model // 2, experts, slots, width // 512 * 256 + 256
        ),
        out_shape=(
            jax.ShapeDtypeStruct((levels, 8 * slots, width), bf16),
            jax.ShapeDtypeStruct((levels, 8 * sub, 8 * slots), bf16),
            jax.ShapeDtypeStruct((levels, 8 * sub, 128), jnp.float32),
        ),
        in_specs=[vmem] * 4 + [hbm] * 2,
        out_specs=(vmem,) * 3,
        scratch_shapes=[
            pltpu.VMEM((levels * 8, sub, model + 128), bf16),
            pltpu.VMEM((model, width), bf16),
            pltpu.VMEM((model, width), bf16),
            pltpu.VMEM((8 * slots, model), bf16),
        ]
        + [dma((2, 2, levels)), dma((2, levels))]
        + [dma((levels * 2,))] * 4
        + [dma((levels,))] * 4
        + [dma((levels * 4,))] * 2
        + [dma((model // LOAD_ROWS,))] * 2,
        compiler_params=pltpu.CompilerParams(
            collective_id=1, has_side_effects=True, vmem_limit_bytes=VMEM_BYTES
        ),
    )(
        stream,
        norm_gain.reshape(1, model),
        router.T,
        expert_ids.T,
        gate,
        up,
    )


def sum_kernel(
    levels, sub, model, half, tile, hidden_ref, placing_ref, weight_ref, down_ref, stream_ref,
    out_ref, part_ref, down_w, core_in, first_in, second_in, z_in, total,
    corner_in, cs, cr, fs, fr, ss, sr, ps, zs, zr, pr, ls,
):
    def load(columns, n):
        return pltpu.make_async_copy(down_ref.at[0, :, columns], down_w.at[:, columns], ls.at[n])

    for n in range(model // tile):
        load(slice(n * tile, (n + 1) * tile), n).start()
    z, x, y, c = place_of()
    x_peer, y_peer, c_peer = at(z, 1 - x, y, c), at(z, x, 1 - y, c), at(z, x, y, 1 - c)
    announce(z, x, y, c, levels)
    f32, bf16 = jnp.float32, jnp.bfloat16
    units = levels * 2
    z_sides = ((1, z > 0), (-1, z < levels - 1))
    c_copies, stage2, stage3 = {}, {}, {}

    def place(u):
        return level_at(z, levels - 1 - u // 2, levels), u // 2, u % 2

    def terms_of(u):
        k, r, h = place(u)
        weight = jnp.concatenate([weight_ref[k]] * (tile // 128), axis=1)
        hidden = hidden_ref[k]
        placing = placing_ref[k]

        def one(j, carry):
            columns = pl.ds(pl.multiple_of(h * half + j * tile, tile), tile)
            if r == 0:
                load(columns, h * (half // tile) + j).wait()
            rows = jnp.dot(hidden, down_w[:, columns], preferred_element_type=f32).astype(bf16)
            spread = jnp.dot(placing, rows, preferred_element_type=f32)
            inner = pl.ds(pl.multiple_of(j * tile, tile), tile)
            part_ref[k, h, :, :, :, :, inner] = (
                (spread * weight).astype(bf16).reshape(2, 2, 2, sub, tile)
            )
            return carry

        lax.fori_loop(0, half // tile, one, 0)
        if u == 0:
            meet(z, levels)
        c_copies[u] = start_send(
            part_ref.at[k, h, :, :, 1 - c], core_in.at[r, h], cs.at[u], cr.at[u], c_peer
        )

    direct = {}
    inside = jnp.minimum(z * (levels - 1 - z), 1)

    def corner_copy(u, side, slot):
        k, _, h = place(u)
        if slot is None:
            slot = side * inside + 2 * (1 - inside)
        return pltpu.make_async_remote_copy(
            src_ref=part_ref.at[k, h, 1 - x, 1 - y, c],
            dst_ref=corner_in.at[slot, h],
            send_sem=ps.at[u],
            recv_sem=pr.at[slot, h],
            device_id=at(z + z_sides[side][0], x, y, c),
            device_id_type=MESH,
        )

    def corner_add(u, slot):
        k, _, h = place(u)
        corner_copy(u, 0, slot).wait_recv()
        part_ref[k, h, 1 - x, 1 - y, c] = (
            part_ref[k, h, 1 - x, 1 - y, c].astype(f32) + corner_in[slot, h].astype(f32)
        ).astype(bf16)

    def first_of(u):
        k, r, h = place(u)
        c_copies[u].wait_recv()
        for bx in range(2):
            for by in range(2):
                part_ref[k, h, bx, by, c] = (
                    part_ref[k, h, bx, by, c].astype(f32) + core_in[r, h, bx, by].astype(f32)
                ).astype(bf16)
        if r == levels - 1:
            for side, (_, outer) in enumerate(z_sides):
                pl.when(outer)(functools.partial(corner_add, u, side))
        elif r:
            if r == levels - 2:
                pl.when(inside == 1)(functools.partial(corner_add, u, 2))
            for side, (step, _) in enumerate(z_sides):

                @pl.when((k - z) * step > 0)
                def _():
                    corner_copy(u, side, side if r == levels - 2 else None).start()

            direct[u] = (
                start_send(
                    part_ref.at[k, h, 1 - x, y, c], first_in.at[r, h, 0],
                    fs.at[u], fr.at[u], x_peer,
                ),
                start_send(
                    part_ref.at[k, h, x, 1 - y, c], first_in.at[r, h, 1],
                    ss.at[u], sr.at[u], y_peer,
                ),
            )
            return
        if h:
            src, peer = part_ref.at[k, h, 1 - x, :, c], x_peer
        else:
            src, peer = part_ref.at[k, h, :, 1 - y, c], y_peer
        stage2[u] = start_send(src, first_in.at[r, h], fs.at[u], fr.at[u], peer)

    def second_of(u):
        k, r, h = place(u)
        if u not in stage2:
            return
        stage2[u].wait_recv()
        bx, by, other, peer = (x, 1 - y, 1 - y, y_peer) if h else (1 - x, y, 1 - x, x_peer)
        part_ref[k, h, bx, by, c] = (
            part_ref[k, h, bx, by, c].astype(f32) + first_in[r, h, other].astype(f32)
        ).astype(bf16)
        stage3[u] = start_send(
            part_ref.at[k, h, bx, by, c], second_in.at[r, h], ss.at[u], sr.at[u], peer
        )

    def z_copy(u, side):
        k, _, h = place(u)
        return pltpu.make_async_remote_copy(
            src_ref=part_ref.at[k, h, x, y, c],
            dst_ref=z_in.at[side, k, h],
            send_sem=zs.at[u],
            recv_sem=zr.at[side, k, h],
            device_id=at(z + z_sides[side][0], x, y, c),
            device_id_type=MESH,
        )

    def z_send(u, with_outer):
        k, _, h = place(u)
        for side, (step, outer) in enumerate(z_sides):
            right_way = (k - z) * step > 0

            @pl.when(jnp.logical_and(right_way, outer if with_outer else jnp.logical_not(outer)))
            def _():
                if with_outer:
                    z_copy(u, side).wait_recv()
                    part_ref[k, h, x, y, c] = (
                        part_ref[k, h, x, y, c].astype(f32) + z_in[side, k, h].astype(f32)
                    ).astype(bf16)
                z_copy(u, side).start()

    def third_of(u):
        k, r, h = place(u)
        value = part_ref[k, h, x, y, c].astype(f32)
        if u in direct:
            for i, copy in enumerate(direct[u]):
                copy.wait_recv()
                value = value + first_in[r, h, i].astype(f32)
        else:
            stage3[u].wait_recv()
            value = value + first_in[r, h, y if h else x].astype(f32)
            value = value + second_in[r, h].astype(f32)
        if r < levels - 1:
            part_ref[k, h, x, y, c] = value.astype(bf16)
            z_send(u, False)
        else:
            total[h] = stream_ref[:, h * half : (h + 1) * half].astype(f32) + value

    second_lag, direct_lag, third_lag = 2, 2, 4
    terms_of(0)
    for step in range(units + third_lag):
        if step < units:
            first_of(step)
        if step + 1 < units:
            terms_of(step + 1)
        if 0 <= step - second_lag < units:
            second_of(step - second_lag)
        for u in range(units):
            outer = 0 < u // 2 < levels - 1
            lag = direct_lag if outer else third_lag
            if step == u + lag:
                third_of(u)
            if u < units - 2 and step == u + lag + (2, 4, 0)[u // 2]:
                z_send(u, True)
    for u in range(units - 2, units):
        h = u % 2
        for side, (_, outer) in enumerate(z_sides):

            @pl.when(outer)
            def _():
                z_copy(u, side).wait_recv()
                total[h] += z_in[side, z, h].astype(f32)

        out_ref[:, h * half : (h + 1) * half] = total[h].astype(bf16)
    for u in range(units):
        c_copies[u].wait_send()
        for copy in direct[u] if u in direct else (stage2[u], stage3[u]):
            copy.wait_send()
        if u in direct:
            corner_copy(u, 0, 0).wait_send()
        if u < units - 2:
            z_copy(u, 0).wait_send()


def sum_terms(hidden, placing, weight, down, stream, levels):
    sub, model = stream.shape
    half = model // 2
    tile = 1024
    vmem = pl.BlockSpec(memory_space=pltpu.VMEM)
    dma = pltpu.SemaphoreType.DMA
    bf16 = jnp.bfloat16
    return pl.pallas_call(
        functools.partial(sum_kernel, levels, sub, model, half, tile),
        out_shape=jax.ShapeDtypeStruct((sub, model), bf16),
        in_specs=[vmem] * 3 + [pl.BlockSpec(memory_space=pl.ANY), vmem],
        out_specs=vmem,
        scratch_shapes=[
            pltpu.VMEM((levels, 2, 2, 2, 2, sub, half), bf16),
            pltpu.VMEM(down.shape[1:], bf16),
            pltpu.VMEM((levels, 2, 2, 2, sub, half), bf16),
            pltpu.VMEM((levels, 2, 2, sub, half), bf16),
            pltpu.VMEM((levels, 2, sub, half), bf16),
            pltpu.VMEM((2, levels, 2, sub, half), bf16),
            pltpu.VMEM((2, sub, half), jnp.float32),
            pltpu.VMEM((3, 2, sub, half), bf16),
        ]
        + [dma((levels * 2,))] * 8
        + [dma((2, levels, 2)), dma((3, 2)), dma((model // tile,))],
        compiler_params=pltpu.CompilerParams(
            collective_id=2, has_side_effects=True, vmem_limit_bytes=VMEM_BYTES
        ),
    )(hidden, placing, weight, down, stream)


def on_device(
    levels,
    queries,
    keys,
    values,
    resid_in,
    span_order,
    out_weight,
    norm_gain,
    router,
    expert_ids,
    w_gate,
    w_up,
    w_down,
):
    stream = attend(queries, keys, values, span_order, resid_in, out_weight, levels)
    hidden, placing, weight = hidden_units(
        stream, norm_gain, router, expert_ids, w_gate, w_up, levels
    )
    return sum_terms(hidden, placing, weight, w_down, stream, levels)


def solution(mesh):
    placed = (
        P("ctx", "exp"),
        P("ctx", "exp"),
        P("ctx", "exp"),
        P(("ctx", "exp"), None),
        P(),
        P("exp", None),
        P(),
        P(),
        P(("ctx", "exp"), None),
        P("exp", None, "ctx"),
        P("exp", None, "ctx"),
        P("exp", "ctx", None),
    )
    levels = mesh.shape["ctx"] // 2

    def body(queries, keys, values, resid_in, *rest):
        blocks = resid_in.size * mesh.size * 2
        small = mesh.shape["exp"] == 4 and levels == 4 and blocks * 4 <= VMEM_BYTES
        local = functools.partial(on_device, levels) if small else on_device_xla
        return local(queries, keys, values, resid_in, *rest)

    return jax.shard_map(
        body, mesh=mesh, in_specs=placed, out_specs=P(("ctx", "exp"), None), check_vma=False
    )
```
